32 devices in a mesh: blk: 16 (over z, x, core), grp: 2 (over y).
Axes of the slice: x: 2, y: 2, z: 4, core: 2. Of those that a mesh axis runs over, the one named last changes fastest.
Arguments:
- embeddings: bfloat16 [32768, 1024], P(('blk', 'grp')), may hold values from -6 to 6
Outputs:
- tile_max: float32 [32768, 40], P(('blk', 'grp'))
The draws below stay inside these ranges and needn't reach their ends.
All inputs are finite; a program needn't handle non-finite values.
Results may differ from the reference program's by a relative error of at most 0.0017.
Values may be sent and summed in bfloat16 or wider, within the bound.
No kernel may reach another device: no remote copies, remote signals or barrier semaphores. Data moves between devices by JAX's collectives and lax.ppermute only.
A program may use at most 64 MiB of HBM per device.

```python
import jax
import jax.numpy as jnp
from jax import lax

D = 1024
R_DEV = 1024
TILES = 8
BLOCKS = 32
ROWS = 32768


def steps_of(key, extent, split, least, largest):
    loudness = 1.0
    for axis_at, shards_of in split:
        heights = jax.random.uniform(jax.random.fold_in(jax.random.fold_in(key, 6), axis_at), (shards_of,), jnp.float32, least / len(split), largest / len(split))
        loudness = loudness * jnp.repeat(jnp.exp(heights), extent[axis_at] // shards_of).reshape((-1,) + (1,) * (len(extent) - 1 - axis_at))
    return loudness


def normal_values(own_key, dims, deviation, most, split=(), held_as=jnp.bfloat16):
    array = jax.random.normal(own_key, dims, jnp.float32) * deviation
    if len(split) > 0:
        array = steps_of(own_key, dims, split, -0.22, 0.18) * array
    return jnp.clip(array, min=-most, max=most).astype(held_as)


def setup_inputs(seed: int = 0) -> dict:
    splits = jax.random.split(jax.random.key(seed), 2)
    return {
        "embeddings": normal_values(splits[0], (ROWS, D), 1.0, 6.0, ((0, 32),)),
    }


def tile_rows(scores):
    count = scores.shape[0]
    return lax.optimization_barrier(jnp.max(scores.reshape(count, count // 128, 128), axis=-1))

def tile_columns(scores):
    count = scores.shape[0]
    return jnp.transpose(lax.optimization_barrier(jnp.max(scores.reshape(count // 128, 128, count), axis=1)))

def reference(embeddings):
    values = embeddings.astype(jnp.float32)
    unit = (values * lax.rsqrt(lax.optimization_barrier(jnp.mean(values * values, axis=-1, keepdims=True)) + 1e-06)).astype(jnp.bfloat16)
    blocks = unit.reshape(BLOCKS, R_DEV, D)
    next_one = jnp.roll(blocks, -1, axis=0)
    next_two = jnp.roll(blocks, -2, axis=0)
    scale = 1.0 / D ** 0.5
    same = jnp.arange(R_DEV)[:, None] == jnp.arange(R_DEV)[None, :]

    def score(queries, keys):
        return lax.dot_general(queries, keys, (((1,), (1,)), ((), ())), preferred_element_type=jnp.float32) * scale

    def per_block(triple):
        queries, first, second = triple
        own = jnp.where(same, -jnp.inf, score(queries, queries))
        one = score(queries, first)
        two = score(queries, second)
        return (tile_rows(own), tile_rows(one), tile_rows(two), tile_columns(one), tile_columns(two))
    own_max, one_max, two_max, col_one, col_two = lax.map(per_block, (blocks, next_one, next_two))
    back_one = jnp.roll(col_one, 1, axis=0)
    back_two = jnp.roll(col_two, 2, axis=0)
    joined = jnp.concatenate([back_two, back_one, own_max, one_max, two_max], axis=2)
    return joined.reshape(ROWS, 5 * TILES)
```

```python
import functools

import jax
import jax.numpy as jnp
from jax import lax
from jax.experimental import pallas as pl
from jax.experimental.pallas import tpu as pltpu
from jax.sharding import PartitionSpec as P

AXES = ("blk", "grp")
TILE = 128
OFFSETS = 5


def unit_of(rows):
    values = rows.astype(jnp.float32)
    mean = jnp.mean(values * values, axis=-1, keepdims=True)
    return (values * lax.rsqrt(mean + 1e-06)).astype(jnp.bfloat16)


def scores(left, right):
    return lax.dot_general(left, right, (((1,), (1,)), ((), ())), preferred_element_type=jnp.float32)


def best(left, right, scale):
    found = []
    for t in range(left.shape[0] // TILE):
        s = scores(left[t * TILE : (t + 1) * TILE, :], right)
        found.append(jnp.max(s, axis=0, keepdims=True))
    return jnp.concatenate(found, axis=0) * scale


def own_kernel(scale, rows_ref, unit_ref, own_ref):
    unit_ref[...] = unit_of(rows_ref[...])
    same = lax.broadcasted_iota(jnp.int32, (TILE, TILE), 0) == lax.broadcasted_iota(
        jnp.int32, (TILE, TILE), 1
    )
    count = rows_ref.shape[0]
    for t in range(count // TILE):
        at = t * TILE
        s = scores(unit_ref[at : at + TILE, :], unit_ref[...])
        blocks = [s[:, :at], jnp.where(same, -jnp.inf, s[:, at : at + TILE]), s[:, at + TILE :]]
        s = jnp.concatenate([b for b in blocks if b.shape[1]], axis=1)
        own_ref[t : t + 1, :] = jnp.max(s, axis=0, keepdims=True) * scale


def partner_kernel(scale, rows_ref, unit_ref, partner_ref, max_ref):
    partner_ref[...] = unit_of(rows_ref[...])
    max_ref[...] = best(partner_ref[...], unit_ref[...], scale)


def far_kernel(scale, rows_ref, unit_ref, partner_ref, far_ref, own_far_ref, far_own_ref, partner_far_ref):
    far_ref[...] = unit_of(rows_ref[...])
    own_far_ref[...] = best(far_ref[...], unit_ref[...], scale)
    partner_far_ref[...] = best(far_ref[...], partner_ref[...], scale)
    far_own_ref[...] = best(unit_ref[...], far_ref[...], scale)


def half_kernel(scale, role_ref, even_ref, odd_ref, unit_ref, far_ref, half_tiles_ref, half_rows_ref, half_ref):
    turn = role_ref[0]
    step = role_ref[1]
    middle = jnp.logical_or(turn == 1, turn == 2)

    @pl.when(jnp.logical_and(step == 0, middle))
    def _():
        half_ref[...] = unit_of(even_ref[...])
        half_tiles_ref[...] = best(half_ref[...], far_ref[...], scale)
        half_rows_ref[...] = best(far_ref[...], half_ref[...], scale)

    @pl.when(jnp.logical_and(step == 1, jnp.logical_not(middle)))
    def _():
        half_ref[...] = unit_of(odd_ref[...])
        half_tiles_ref[...] = best(half_ref[...], unit_ref[...], scale)
        half_rows_ref[...] = best(unit_ref[...], half_ref[...], scale)


def join_kernel(
    role_ref, own_ref, own_far_ref, own_partner_ref, half_tiles_ref, back_far_ref, back_tiles_ref,
    back_partner_ref, back_even_ref, back_odd_ref, out_ref, held_ref,
):
    turn = role_ref[0]
    step = role_ref[1]
    middle = jnp.logical_or(turn == 1, turn == 2)
    tiles, count = own_ref.shape
    half = count // 2

    def put(slots, value):
        slot = slots[0]
        for i in range(1, 4):
            slot = jnp.where(turn == i, slots[i], slot)
        held_ref[pl.ds(pl.multiple_of(slot * tiles, tiles), tiles), :] = value

    put((2, 2, 2, 2), own_ref[...])
    put((3, 0, 4, 1), own_far_ref[...])
    put((4, 4, 0, 0), own_partner_ref[...])
    put((0, 1, 3, 4), back_far_ref[...])

    @pl.when(middle)
    def _():
        put((0, 3, 1, 0), back_partner_ref[...])

    @pl.when(jnp.logical_and(jnp.logical_not(middle), step == 0))
    def _():
        put((1, 1, 1, 3), jnp.concatenate([back_even_ref[...], back_odd_ref[...]], axis=1))

    @pl.when(jnp.logical_and(jnp.logical_not(middle), step == 1))
    def _():
        put((1, 1, 1, 3), jnp.concatenate([back_tiles_ref[...], half_tiles_ref[...]], axis=0))

    out_ref[...] = jnp.transpose(held_ref[...])


def call(kernel, outs, *operands, scratch=(), scalars=0):
    in_specs = [
        pl.BlockSpec(memory_space=pltpu.SMEM if i < scalars else pltpu.VMEM) for i in range(len(operands))
    ]
    shapes = tuple(jax.ShapeDtypeStruct(s, d) for s, d in outs)
    specs = tuple(pl.BlockSpec(memory_space=pltpu.VMEM) for _ in outs)
    return pl.pallas_call(
        kernel, out_shape=shapes, in_specs=in_specs, out_specs=specs, scratch_shapes=list(scratch)
    )(*operands)


def body(embeddings):
    count, width = embeddings.shape
    blocks = lax.axis_size(AXES[0]) * lax.axis_size(AXES[1])
    columns = blocks // 4
    assert blocks % 8 == 0
    scale = 1.0 / width**0.5
    tiles, half = count // TILE, count // 2
    f32, bf16 = jnp.float32, jnp.bfloat16

    at = lambda column, turn: column % columns * 4 + turn
    far, swap, even, odd, odd_back = [], [], [], [], []
    for q in range(columns):
        far += [(at(q, 1), at(q, 0)), (at(q, 2), at(q, 3))]
        far += [(at(q, 3), at(q + 1, 1)), (at(q, 0), at(q - 1, 2))]
        swap += [(at(q, 0), at(q, 2)), (at(q, 2), at(q, 0)), (at(q, 1), at(q, 3)), (at(q, 3), at(q, 1))]
        if q % 2 == 0:
            even += [(at(q, 0), at(q, 1)), (at(q, 3), at(q, 2))]
        else:
            odd += [(at(q, 1), at(q, 0)), (at(q, 2), at(q, 3))]
            odd_back += [(at(q, 0), at(q - 1, 3)), (at(q, 3), at(q + 1, 0))]
    turned = lambda pairs: [(b, a) for a, b in pairs]
    send = lambda value, pairs: lax.ppermute(value, AXES, pairs)

    index = lax.axis_index(AXES)
    role = jnp.stack([index % 4, index // 4 % 2]).astype(jnp.int32)

    cuts = [(half, count), (0, half // 2), (half // 2, half)]
    parts, first_half, embeddings = lax.optimization_barrier(
        ({c: embeddings[c[0] : c[1]] for c in cuts}, embeddings[:half], embeddings)
    )
    far_rows = {c: send(parts[c], far) for c in cuts}
    even_rows = send(first_half, even)
    partner_rows = send(embeddings, swap)
    unit, own = call(
        functools.partial(own_kernel, scale), [((count, width), bf16), ((tiles, count), f32)], embeddings
    )
    partner, own_partner = call(
        functools.partial(partner_kernel, scale),
        [((count, width), bf16), ((tiles, count), f32)],
        partner_rows,
        unit,
    )
    first, own_partner = lax.optimization_barrier((far_rows[cuts[0]], own_partner))
    far_rows[cuts[0]] = first
    odd_rows = send(first, odd)
    pieces = {}
    for c in cuts:
        n = c[1] - c[0]
        pieces[c] = call(
            functools.partial(far_kernel, scale),
            [((n, width), bf16), ((n // TILE, count), f32), ((tiles, n), f32), ((n // TILE, count), f32)],
            far_rows[c],
            unit,
            partner,
        )
    ordered = [pieces[c] for c in sorted(cuts)]
    far_unit = jnp.concatenate([p[0] for p in ordered], axis=0)
    own_far = jnp.concatenate([p[1] for p in ordered], axis=0)
    far_own = jnp.concatenate([p[2] for p in ordered], axis=1)
    partner_far = jnp.concatenate([p[3] for p in ordered], axis=0)

    half_tiles, half_rows = call(
        functools.partial(half_kernel, scale),
        [((half // TILE, count), f32), ((tiles, half), f32)],
        role,
        even_rows,
        odd_rows,
        unit,
        far_unit,
        scalars=1,
        scratch=[pltpu.VMEM((half, width), bf16)],
    )
    back_far = send(far_own, turned(far))
    back_tiles = send(half_tiles, turned(far))
    back_partner = send(partner_far, [p for p in swap if p[0] % 4 in (0, 3)])
    back_even = send(half_rows, turned(even))
    back_odd = send(half_rows, odd_back)

    (out,) = call(
        join_kernel,
        [((count, OFFSETS * tiles), f32)],
        role,
        own,
        own_far,
        own_partner,
        half_tiles,
        back_far,
        back_tiles,
        back_partner,
        back_even,
        back_odd,
        scalars=1,
        scratch=[pltpu.VMEM((OFFSETS * tiles, count), f32)],
    )
    return out


def solution(mesh):
    return jax.shard_map(
        body,
        mesh=mesh,
        in_specs=(P(AXES, None),),
        out_specs=P(AXES, None),
        check_vma=False,
    )
```

```python
import functools

import jax
import jax.numpy as jnp
from jax import lax
from jax.experimental import pallas as pl
from jax.experimental.pallas import tpu as pltpu
from jax.sharding import PartitionSpec as P

AXES = ("blk", "grp")
TILE = 128
STEP = 256
OFFSETS = 5
VMEM_LIMIT = 16 << 20
F32, BF16 = jnp.float32, jnp.bfloat16


def unit_of(rows):
    values = rows.astype(F32)
    mean = jnp.mean(values * values, axis=-1, keepdims=True)
    return (values * lax.rsqrt(mean + 1e-06)).astype(BF16)


def scores(left, right):
    return lax.dot_general(left, right, (((1,), (1,)), ((), ())), preferred_element_type=F32)


def best(scale, left, right, right_ref, right_at=0, left_ref=None, left_at=0, same=None):
    rows, keys = left.shape[0], right.shape[0]
    for m in range(0, rows, STEP):
        for n in range(0, keys, STEP):
            s = scores(left[m : m + STEP, :], right[n : n + STEP, :])
            if same is not None and m == n:
                s = jnp.where(same, -jnp.inf, s)
            tiles = jnp.max(s.reshape(STEP // TILE, TILE, STEP), axis=1)
            at = right_at + m // TILE
            right_ref[at : at + STEP // TILE, n : n + STEP] = tiles * scale
            if left_ref is not None:
                for t in range(STEP // TILE):
                    tile = jnp.max(s[:, t * TILE : (t + 1) * TILE], axis=1)
                    at = n // TILE + t
                    left_ref[at : at + 1, left_at + m : left_at + m + STEP] = tile.reshape(1, STEP) * scale


def cut_kernel(rows_ref, high_ref, low_ref, high_sem, low_sem):
    half = high_ref.shape[0]
    high = pltpu.make_async_copy(rows_ref.at[half:, :], high_ref, high_sem)
    low = pltpu.make_async_copy(rows_ref.at[:half, :], low_ref, low_sem)
    high.start()
    low.start()
    high.wait()
    low.wait()


def own_kernel(scale, rows_ref, unit_ref, own_ref):
    unit_ref[...] = unit_of(rows_ref[...])
    same = lax.broadcasted_iota(jnp.int32, (STEP, STEP), 0) == lax.broadcasted_iota(
        jnp.int32, (STEP, STEP), 1
    )
    best(scale, unit_ref, unit_ref, own_ref, same=same)


def partner_kernel(scale, rows_ref, unit_ref, partner_ref, max_ref):
    partner_ref[...] = unit_of(rows_ref[...])
    best(scale, partner_ref, unit_ref, max_ref)


def far_kernel(scale, rows_ref, unit_ref, partner_ref, far_ref, own_far_ref, far_own_ref, partner_far_ref):
    far_ref[...] = unit_of(rows_ref[...])
    best(scale, far_ref, unit_ref, own_far_ref, left_ref=far_own_ref)
    best(scale, far_ref, partner_ref, partner_far_ref)


def half_kernel(
    scale, role_ref, even_ref, odd_ref, unit_ref, low_ref, high_ref, cross_ref, back_ref, tiles_ref, half_ref
):
    turn, step = role_ref[0], role_ref[1]
    middle = jnp.logical_or(turn == 1, turn == 2)
    half = half_ref.shape[0]

    @pl.when(jnp.logical_and(step == 0, middle))
    def _():
        half_ref[...] = unit_of(even_ref[...])
        best(scale, half_ref, low_ref, tiles_ref, left_ref=back_ref)
        cross_ref[: half // TILE, :] = tiles_ref[:, :half]
        best(scale, half_ref, high_ref, tiles_ref, left_ref=back_ref.at[half // TILE :, :])
        cross_ref[half // TILE :, :] = tiles_ref[:, :half]

    @pl.when(jnp.logical_and(step == 1, jnp.logical_not(middle)))
    def _():
        half_ref[...] = unit_of(odd_ref[...])
        best(scale, half_ref, unit_ref, tiles_ref, left_ref=cross_ref)


def join_kernel(
    role_ref, own_ref, own_partner_ref, own_high_ref, own_low_ref, tiles_ref, far_high_ref, far_low_ref,
    partner_high_ref, partner_low_ref, cross_ref, even_ref, out_ref,
):
    turn, step = role_ref[0], role_ref[1]
    middle = jnp.logical_or(turn == 1, turn == 2)
    tiles, count = own_ref.shape
    half = count // 2

    def put(slots, *values):
        slot = slots[0]
        for i in range(1, 4):
            slot = jnp.where(turn == i, slots[i], slot)
        at = pl.multiple_of(slot * tiles, tiles)
        out_ref[pl.ds(at, tiles), :] = jnp.concatenate(values[1:], axis=values[0])

    put((2, 2, 2, 2), 0, own_ref[...])
    put((4, 4, 0, 0), 0, own_partner_ref[...])
    put((3, 0, 4, 1), 0, own_low_ref[...], own_high_ref[...])
    put((0, 1, 3, 4), 1, far_low_ref[...], far_high_ref[...])

    @pl.when(middle)
    def _():
        put((0, 3, 1, 0), 0, partner_low_ref[...], partner_high_ref[...])

    @pl.when(jnp.logical_and(jnp.logical_not(middle), step == 0))
    def _():
        put((1, 1, 1, 3), 1, even_ref[...], cross_ref[...])

    @pl.when(jnp.logical_and(jnp.logical_not(middle), step == 1))
    def _():
        across = [cross_ref[: tiles // 2, :], cross_ref[tiles // 2 :, :]]
        put((1, 1, 1, 3), 0, jnp.concatenate(across, axis=1), tiles_ref[...])


def call(kernel, outs, *operands, near=(), scratch=(), hbm=False, last=False):
    near = set(near)
    specs = []
    placed = []
    for i, value in enumerate(operands):
        if value.dtype == jnp.int32:
            specs.append(pl.BlockSpec(memory_space=pltpu.SMEM))
        elif hbm:
            specs.append(pl.BlockSpec(memory_space=pltpu.HBM))
            value = pltpu.with_memory_space_constraint(value, pltpu.HBM)
        else:
            specs.append(pl.BlockSpec(memory_space=pltpu.VMEM))
            if i in near:
                value = pltpu.with_memory_space_constraint(value, pltpu.VMEM)
        placed.append(value)
    shapes, out_specs = [], []
    for shape, dtype in outs:
        if hbm:
            shapes.append(jax.ShapeDtypeStruct(shape, dtype))
            out_specs.append(pl.BlockSpec(memory_space=pl.ANY))
        else:
            shapes.append(pltpu.VMEM(shape, dtype) if near and not last else jax.ShapeDtypeStruct(shape, dtype))
            out_specs.append(pl.BlockSpec(memory_space=pltpu.VMEM))
    return pl.pallas_call(
        kernel,
        out_shape=shapes,
        in_specs=specs,
        out_specs=out_specs,
        scratch_shapes=list(scratch),
        compiler_params=pltpu.CompilerParams(vmem_limit_bytes=VMEM_LIMIT),
    )(*placed)


def body(embeddings):
    count, width = embeddings.shape
    blocks = lax.axis_size(AXES[0]) * lax.axis_size(AXES[1])
    columns = blocks // 4
    assert blocks % 8 == 0 and count % (2 * STEP) == 0
    scale = 1.0 / width**0.5
    tiles, half = count // TILE, count // 2

    at = lambda column, turn: column % columns * 4 + turn
    far, swap, even, odd, cross = [], [], [], [], []
    for q in range(columns):
        far += [(at(q, 1), at(q, 0)), (at(q, 2), at(q, 3))]
        far += [(at(q, 3), at(q + 1, 1)), (at(q, 0), at(q - 1, 2))]
        swap += [(at(q, 0), at(q, 2)), (at(q, 2), at(q, 0)), (at(q, 1), at(q, 3)), (at(q, 3), at(q, 1))]
        if q % 2 == 0:
            even += [(at(q, 0), at(q, 1)), (at(q, 3), at(q, 2))]
            cross += [(at(q, 1), at(q - 1, 3)), (at(q, 2), at(q + 1, 0))]
        else:
            odd += [(at(q, 1), at(q, 0)), (at(q, 2), at(q, 3))]
            cross += [(at(q, 0), at(q - 1, 3)), (at(q, 3), at(q + 1, 0))]
    turned = lambda pairs: [(b, a) for a, b in pairs]
    send = lambda value, pairs: lax.ppermute(value, AXES, pairs)

    index = lax.axis_index(AXES)
    role = jnp.stack([index % 4, index // 4 % 2]).astype(jnp.int32)

    high, low = call(
        cut_kernel,
        [((half, width), BF16)] * 2,
        embeddings,
        hbm=True,
        scratch=[pltpu.SemaphoreType.DMA, pltpu.SemaphoreType.DMA],
    )
    high_rows = send(high, far)
    low_rows = send(low, far)
    partner_rows = send(embeddings, swap)

    embeddings, high, low = lax.optimization_barrier((embeddings, high, low))
    unit, own = call(
        functools.partial(own_kernel, scale), [((count, width), BF16), ((tiles, count), F32)], embeddings, near=(9,)
    )
    partner, own_partner = call(
        functools.partial(partner_kernel, scale),
        [((count, width), BF16), ((tiles, count), F32)],
        partner_rows,
        unit,
        near=(0, 1),
    )
    high_rows, low, own_partner = lax.optimization_barrier((high_rows, low, own_partner))
    odd_rows = send(high_rows, odd)
    even_rows = send(low, even)
    far_of = lambda rows: call(
        functools.partial(far_kernel, scale),
        [((half, width), BF16), ((tiles // 2, count), F32), ((tiles, half), F32), ((tiles // 2, count), F32)],
        rows,
        unit,
        partner,
        near=(0, 1, 2),
    )
    high_unit, own_high, high_own, partner_high = far_of(high_rows)
    low_unit, own_low, low_own, partner_low = far_of(low_rows)

    halves = [p for p in swap if p[0] % 4 in (0, 3)]
    far_high = send(high_own, turned(far))
    back_high = send(partner_high, halves)
    far_low = send(low_own, turned(far))
    back_low = send(partner_low, halves)
    crossing, back, half_tiles = call(
        functools.partial(half_kernel, scale),
        [((tiles, half), F32), ((tiles, half), F32), ((tiles // 2, count), F32)],
        role,
        even_rows,
        odd_rows,
        unit,
        low_unit,
        high_unit,
        near=(1, 2, 3, 4, 5),
        scratch=[pltpu.VMEM((half, width), BF16)],
    )
    crossed = send(crossing, cross)
    back_even = send(back, turned(even))

    (out,) = call(
        join_kernel,
        [((OFFSETS * tiles, count), F32)],
        role,
        own,
        own_partner,
        own_high,
        own_low,
        half_tiles,
        far_high,
        far_low,
        back_high,
        back_low,
        crossed,
        back_even,
        near=range(1, 12),
        last=True,
    )
    return jnp.transpose(out)


def solution(mesh):
    return jax.shard_map(
        body,
        mesh=mesh,
        in_specs=(P(AXES, None),),
        out_specs=P(AXES, None),
        check_vma=False,
    )
```

```python
import functools

import jax
import jax.numpy as jnp
from jax import lax
from jax.experimental import pallas as pl
from jax.experimental.pallas import tpu as pltpu
from jax.sharding import PartitionSpec as P

AXES = ("blk", "grp")
TILE = 128
STEP = 256
OFFSETS = 5
VMEM_LIMIT = 16 << 20
F32, BF16 = jnp.float32, jnp.bfloat16


def unit_of(rows):
    values = rows.astype(F32)
    mean = jnp.mean(values * values, axis=-1, keepdims=True)
    return (values * lax.rsqrt(mean + 1e-06)).astype(BF16)


def scores(left, right):
    return lax.dot_general(left, right, (((1,), (1,)), ((), ())), preferred_element_type=F32)


def best(scale, left, right, right_ref, right_at=0, left_ref=None, left_at=0, same=None):
    rows, keys = left.shape[0], right.shape[0]
    for m in range(0, rows, STEP):
        for n in range(0, keys, STEP):
            s = scores(left[m : m + STEP, :], right[n : n + STEP, :])
            if same is not None and m == n:
                s = jnp.where(same, -jnp.inf, s)
            tiles = jnp.max(s.reshape(STEP // TILE, TILE, STEP), axis=1)
            at = right_at + m // TILE
            right_ref[at : at + STEP // TILE, n : n + STEP] = tiles * scale
            if left_ref is not None:
                for t in range(STEP // TILE):
                    tile = jnp.max(s[:, t * TILE : (t + 1) * TILE], axis=1)
                    at = n // TILE + t
                    left_ref[at : at + 1, left_at + m : left_at + m + STEP] = tile.reshape(1, STEP) * scale


def place(role_ref):
    turn = lax.rem(role_ref[0], 4)
    step = lax.rem(lax.div(role_ref[0], 4), 2)
    return turn, step, jnp.logical_or(turn == 1, turn == 2)


def cut_kernel(rows_ref, high_ref, low_ref, high_sem, low_sem):
    half = high_ref.shape[0]
    high = pltpu.make_async_copy(rows_ref.at[half:, :], high_ref, high_sem)
    low = pltpu.make_async_copy(rows_ref.at[:half, :], low_ref, low_sem)
    high.start()
    low.start()
    high.wait()
    low.wait()


def own_kernel(scale, high_ref, low_ref, unit_ref, own_ref):
    half = low_ref.shape[0]
    unit_ref[:half, :] = unit_of(low_ref[...])
    unit_ref[half:, :] = unit_of(high_ref[...])
    same = lax.broadcasted_iota(jnp.int32, (STEP, STEP), 0) == lax.broadcasted_iota(
        jnp.int32, (STEP, STEP), 1
    )
    best(scale, unit_ref, unit_ref, own_ref, same=same)


def partner_kernel(scale, rows_ref, unit_ref, partner_ref, max_ref):
    partner_ref[...] = unit_of(rows_ref[...])
    best(scale, partner_ref, unit_ref, max_ref)


def far_kernel(
    scale, rows_ref, unit_ref, partner_ref, far_ref, own_far_ref, far_own_ref, partner_far_ref
):
    far_ref[...] = unit_of(rows_ref[...])
    best(scale, far_ref, unit_ref, own_far_ref, left_ref=far_own_ref)
    best(scale, far_ref, partner_ref, partner_far_ref)


def last_kernel(
    scale, role_ref, even_ref, odd_ref, unit_ref, low_ref, high_ref, low_own_ref, high_own_ref,
    partner_low_ref, partner_high_ref, far_ref, beside_ref, cross_ref, tiles_ref, half_ref,
):
    turn, step, middle = place(role_ref)
    half = half_ref.shape[0]
    across = half // TILE
    tiles = 2 * across
    far_ref[:tiles, :half] = low_own_ref[...]
    far_ref[:tiles, half:] = high_own_ref[...]

    @pl.when(jnp.logical_not(middle))
    def _():
        beside_ref[:across, :] = partner_low_ref[...]
        beside_ref[across:, :] = partner_high_ref[...]

    @pl.when(jnp.logical_and(step == 0, middle))
    def _():
        half_ref[...] = unit_of(even_ref[...])
        best(scale, half_ref, low_ref, far_ref.at[tiles:, :half], left_ref=beside_ref.at[:across, :half])
        best(scale, half_ref, high_ref, far_ref.at[tiles:, half:], left_ref=beside_ref.at[across:, :half])

    @pl.when(jnp.logical_and(step == 1, jnp.logical_not(middle)))
    def _():
        half_ref[...] = unit_of(odd_ref[...])
        best(scale, half_ref, unit_ref, tiles_ref, left_ref=cross_ref)


def join_kernel(
    role_ref, own_ref, own_partner_ref, own_low_ref, own_high_ref, tiles_ref, far_ref, beside_ref, cross_ref, out_ref
):
    turn, step, middle = place(role_ref)
    tiles, count = own_ref.shape
    half = count // 2

    def put(slots, *values):
        slot = slots[0]
        for i in range(1, 4):
            slot = jnp.where(turn == i, slots[i], slot)
        at = pl.multiple_of(slot * tiles, tiles)
        out_ref[pl.ds(at, tiles), :] = jnp.concatenate(values[1:], axis=values[0])

    put((2, 2, 2, 2), 0, own_ref[...])
    put((4, 4, 0, 0), 0, own_partner_ref[...])
    put((3, 0, 4, 1), 0, own_low_ref[...], own_high_ref[...])
    put((0, 1, 3, 4), 0, far_ref[:tiles, :])

    @pl.when(middle)
    def _():
        put((0, 3, 1, 0), 0, beside_ref[...])

    @pl.when(jnp.logical_and(jnp.logical_not(middle), step == 0))
    def _():
        put((1, 1, 1, 3), 1, beside_ref[:, :half], cross_ref[...])

    @pl.when(jnp.logical_and(jnp.logical_not(middle), step == 1))
    def _():
        put((1, 1, 1, 3), 0, far_ref[tiles:, :], tiles_ref[...])


def call(kernel, outs, *operands, scratch=(), source=False, last=False):
    specs, placed = [], []
    for value in operands:
        if value.dtype == jnp.int32:
            specs.append(pl.BlockSpec(memory_space=pltpu.SMEM))
            placed.append(value)
            continue
        space = pltpu.HBM if source else pltpu.VMEM
        specs.append(pl.BlockSpec(memory_space=space))
        placed.append(pltpu.with_memory_space_constraint(value, space))
    return pl.pallas_call(
        kernel,
        out_shape=[jax.ShapeDtypeStruct(*o) if last else pltpu.VMEM(*o) for o in outs],
        in_specs=specs,
        out_specs=[pl.BlockSpec(memory_space=pltpu.VMEM) for _ in outs],
        scratch_shapes=list(scratch),
        compiler_params=pltpu.CompilerParams(vmem_limit_bytes=VMEM_LIMIT),
    )(*placed)


def body(embeddings):
    count, width = embeddings.shape
    blocks = lax.axis_size(AXES[0]) * lax.axis_size(AXES[1])
    columns = blocks // 4
    assert blocks % 8 == 0 and count % (2 * STEP) == 0
    scale = 1.0 / width**0.5
    tiles, half = count // TILE, count // 2

    at = lambda column, turn: column % columns * 4 + turn
    far, swap, even, odd, beside, cross = [], [], [], [], [], []
    for q in range(columns):
        far += [(at(q, 1), at(q, 0)), (at(q, 2), at(q, 3))]
        far += [(at(q, 3), at(q + 1, 1)), (at(q, 0), at(q - 1, 2))]
        swap += [(at(q, 0), at(q, 2)), (at(q, 2), at(q, 0)), (at(q, 1), at(q, 3)), (at(q, 3), at(q, 1))]
        beside += [(at(q, 0), at(q, 2)), (at(q, 3), at(q, 1))]
        if q % 2 == 0:
            even += [(at(q, 0), at(q, 1)), (at(q, 3), at(q, 2))]
            beside += [(at(q, 1), at(q, 0)), (at(q, 2), at(q, 3))]
        else:
            odd += [(at(q, 1), at(q, 0)), (at(q, 2), at(q, 3))]
            cross += [(at(q, 0), at(q - 1, 3)), (at(q, 3), at(q + 1, 0))]
    send = lambda value, pairs: lax.ppermute(value, AXES, pairs)
    role = lax.axis_index(AXES).astype(jnp.int32).reshape(1)

    partner_rows = send(embeddings, swap)
    high, low = call(
        cut_kernel,
        [((half, width), BF16)] * 2,
        embeddings,
        source=True,
        scratch=[pltpu.SemaphoreType.DMA, pltpu.SemaphoreType.DMA],
    )
    high_rows = send(high, far)
    low_rows = send(low, far)
    unit, own = call(
        functools.partial(own_kernel, scale), [((count, width), BF16), ((tiles, count), F32)], high, low
    )
    partner, own_partner = call(
        functools.partial(partner_kernel, scale),
        [((count, width), BF16), ((tiles, count), F32)],
        partner_rows,
        unit,
    )
    high_rows, low, own_partner = lax.optimization_barrier((high_rows, low, own_partner))
    odd_rows = send(high_rows, odd)
    even_rows = send(low, even)
    far_of = lambda rows: call(
        functools.partial(far_kernel, scale),
        [((half, width), BF16), ((tiles // 2, count), F32), ((tiles, half), F32), ((tiles // 2, count), F32)],
        rows,
        unit,
        partner,
    )
    high_unit, own_high, high_own, partner_high = far_of(high_rows)
    low_unit, own_low, low_own, partner_low = far_of(low_rows)
    far_max, beside_max, cross_max, half_tiles = call(
        functools.partial(last_kernel, scale),
        [
            ((tiles + tiles // 2, count), F32),
            ((tiles, count), F32),
            ((tiles, half), F32),
            ((tiles // 2, count), F32),
        ],
        role,
        even_rows,
        odd_rows,
        unit,
        low_unit,
        high_unit,
        low_own,
        high_own,
        partner_low,
        partner_high,
        scratch=[pltpu.VMEM((half, width), BF16)],
    )
    far_max = send(far_max, [(b, a) for a, b in far])
    beside_max = send(beside_max, beside)
    cross_max = send(cross_max, cross)
    (out,) = call(
        join_kernel,
        [((OFFSETS * tiles, count), F32)],
        role,
        own,
        own_partner,
        own_low,
        own_high,
        half_tiles,
        far_max,
        beside_max,
        cross_max,
        last=True,
    )
    return jnp.transpose(out)


def solution(mesh):
    return jax.shard_map(
        body,
        mesh=mesh,
        in_specs=(P(AXES, None),),
        out_specs=P(AXES, None),
        check_vma=False,
    )
```

```python
import functools

import jax
import jax.numpy as jnp
from jax import lax
from jax.experimental import pallas as pl
from jax.experimental.pallas import tpu as pltpu
from jax.sharding import PartitionSpec as P


AXES = ("blk", "grp")
TILE = 128
STEP = 256
OFFSETS = 5
VMEM_LIMIT = 16 << 20
F32, BF16 = jnp.float32, jnp.bfloat16


def unit_of(rows):
    values = rows.astype(F32)
    mean = jnp.mean(values * values, axis=-1, keepdims=True)
    return (values * lax.rsqrt(mean + 1e-06)).astype(BF16)


def scores(left, right):
    return lax.dot_general(left, right, (((1,), (1,)), ((), ())), preferred_element_type=F32)


def best(scale, left, right, right_ref, right_at=0, left_ref=None, left_at=0, same=None):
    rows, keys = left.shape[0], right.shape[0]
    for m in range(0, rows, STEP):
        for n in range(0, keys, STEP):
            s = scores(left[m : m + STEP, :], right[n : n + STEP, :])
            if same is not None and m == n:
                s = jnp.where(same, -jnp.inf, s)
            tiles = jnp.max(s.reshape(STEP // TILE, TILE, STEP), axis=1)
            at = right_at + m // TILE
            right_ref[at : at + STEP // TILE, n : n + STEP] = tiles * scale
            if left_ref is not None:
                for t in range(STEP // TILE):
                    tile = jnp.max(s[:, t * TILE : (t + 1) * TILE], axis=1)
                    at = n // TILE + t
                    left_ref[at : at + 1, left_at + m : left_at + m + STEP] = tile.reshape(1, STEP) * scale


def place(role_ref):
    turn = lax.rem(role_ref[0], 4)
    step = lax.rem(lax.div(role_ref[0], 4), 2)
    return turn, step, jnp.logical_or(turn == 1, turn == 2)


def cut_kernel(at, rows_ref, cut_ref, sem):
    copy = pltpu.make_async_copy(rows_ref.at[at : at + cut_ref.shape[0], :], cut_ref, sem)
    copy.start()
    copy.wait()


def own_kernel(scale, high_ref, low_ref, unit_ref, own_ref):
    half = low_ref.shape[0]
    unit_ref[:half, :] = unit_of(low_ref[...])
    unit_ref[half:, :] = unit_of(high_ref[...])
    same = lax.broadcasted_iota(jnp.int32, (STEP, STEP), 0) == lax.broadcasted_iota(
        jnp.int32, (STEP, STEP), 1
    )
    best(scale, unit_ref, unit_ref, own_ref, same=same)


def partner_kernel(scale, rows_ref, unit_ref, partner_ref, max_ref):
    partner_ref[...] = unit_of(rows_ref[...])
    best(scale, partner_ref, unit_ref, max_ref)


def far_kernel(
    scale, rows_ref, unit_ref, partner_ref, far_ref, own_far_ref, far_own_ref, partner_far_ref
):
    far_ref[...] = unit_of(rows_ref[...])
    best(scale, far_ref, unit_ref, own_far_ref, left_ref=far_own_ref)
    best(scale, far_ref, partner_ref, partner_far_ref)


def last_kernel(
    scale, role_ref, even_ref, odd_ref, unit_ref, low_ref, high_ref, low_own_ref, high_own_ref,
    partner_low_ref, partner_high_ref, far_ref, beside_ref, cross_ref, tiles_ref, half_ref,
):
    _, step, middle = place(role_ref)
    half = half_ref.shape[0]
    across = half // TILE
    tiles = 2 * across
    far_ref[:tiles, :half] = low_own_ref[...]
    far_ref[:tiles, half:] = high_own_ref[...]

    @pl.when(jnp.logical_not(middle))
    def _():
        beside_ref[:across, :] = partner_low_ref[...]
        beside_ref[across:, :] = partner_high_ref[...]

    @pl.when(jnp.logical_and(step == 0, middle))
    def _():
        half_ref[...] = unit_of(even_ref[...])
        best(scale, half_ref, low_ref, far_ref.at[tiles:, :half], left_ref=beside_ref.at[:across, :half])
        best(scale, half_ref, high_ref, far_ref.at[tiles:, half:], left_ref=beside_ref.at[across:, :half])

    @pl.when(jnp.logical_and(step == 1, jnp.logical_not(middle)))
    def _():
        half_ref[...] = unit_of(odd_ref[...])
        best(scale, half_ref, unit_ref, tiles_ref, left_ref=cross_ref)


def join_kernel(
    role_ref, own_ref, own_partner_ref, own_low_ref, own_high_ref, tiles_ref, far_ref, beside_ref, cross_ref, out_ref
):
    turn, step, middle = place(role_ref)
    tiles, count = own_ref.shape
    half = count // 2

    def put(slots, *values):
        slot = slots[0]
        for i in range(1, 4):
            slot = jnp.where(turn == i, slots[i], slot)
        at = pl.multiple_of(slot * tiles, tiles)
        out_ref[pl.ds(at, tiles), :] = jnp.concatenate(values[1:], axis=values[0])

    put((2, 2, 2, 2), 0, own_ref[...])
    put((4, 4, 0, 0), 0, own_partner_ref[...])
    put((3, 0, 4, 1), 0, own_low_ref[...], own_high_ref[...])
    put((0, 1, 3, 4), 0, far_ref[:tiles, :])

    @pl.when(middle)
    def _():
        put((0, 3, 1, 0), 0, beside_ref[...])

    @pl.when(jnp.logical_and(jnp.logical_not(middle), step == 0))
    def _():
        put((1, 1, 1, 3), 1, beside_ref[:, :half], cross_ref[...])

    @pl.when(jnp.logical_and(jnp.logical_not(middle), step == 1))
    def _():
        put((1, 1, 1, 3), 0, far_ref[tiles:, :], tiles_ref[...])


def call(kernel, outs, *operands, scratch=(), source=False, last=False):
    specs, placed = [], []
    for value in operands:
        if value.dtype == jnp.int32:
            specs.append(pl.BlockSpec(memory_space=pltpu.SMEM))
            placed.append(value)
            continue
        space = pltpu.HBM if source else pltpu.VMEM
        specs.append(pl.BlockSpec(memory_space=space))
        placed.append(pltpu.with_memory_space_constraint(value, space))
    return pl.pallas_call(
        kernel,
        out_shape=[jax.ShapeDtypeStruct(*o) if last else pltpu.VMEM(*o) for o in outs],
        in_specs=specs,
        out_specs=[pl.BlockSpec(memory_space=pltpu.VMEM) for _ in outs],
        scratch_shapes=list(scratch),
        compiler_params=pltpu.CompilerParams(vmem_limit_bytes=VMEM_LIMIT),
    )(*placed)


def body(embeddings):
    count, width = embeddings.shape
    blocks = lax.axis_size(AXES[0]) * lax.axis_size(AXES[1])
    columns = blocks // 4
    assert blocks % 8 == 0 and count % (2 * STEP) == 0
    scale = 1.0 / width**0.5
    tiles, half = count // TILE, count // 2

    at = lambda column, turn: column % columns * 4 + turn
    far, swap, even, odd, beside, cross = [], [], [], [], [], []
    for q in range(columns):
        far += [(at(q, 1), at(q, 0)), (at(q, 2), at(q, 3))]
        far += [(at(q, 3), at(q + 1, 1)), (at(q, 0), at(q - 1, 2))]
        swap += [(at(q, 0), at(q, 2)), (at(q, 2), at(q, 0)), (at(q, 1), at(q, 3)), (at(q, 3), at(q, 1))]
        beside += [(at(q, 0), at(q, 2)), (at(q, 3), at(q, 1))]
        if q % 2 == 0:
            even += [(at(q, 0), at(q, 1)), (at(q, 3), at(q, 2))]
            beside += [(at(q, 1), at(q, 0)), (at(q, 2), at(q, 3))]
        else:
            odd += [(at(q, 1), at(q, 0)), (at(q, 2), at(q, 3))]
            cross += [(at(q, 0), at(q - 1, 3)), (at(q, 3), at(q + 1, 0))]

    def send(value, pairs):
        return lax.ppermute(value, AXES, pairs)

    role = lax.axis_index(AXES).astype(jnp.int32).reshape(1)
    role, embeddings = lax.optimization_barrier((role, embeddings))

    def cut(at):
        (part,) = call(
            functools.partial(cut_kernel, at),
            [((half, width), BF16)],
            embeddings,
            source=True,
            scratch=[pltpu.SemaphoreType.DMA],
        )
        return part

    high = cut(half)
    high_rows = send(high, far)
    high, embeddings = lax.optimization_barrier((high, embeddings))
    low = cut(0)
    low_rows = send(low, far)
    low, embeddings = lax.optimization_barrier((low, embeddings))
    partner_rows = send(embeddings, swap)
    unit, own = call(functools.partial(own_kernel, scale), [((count, width), BF16), ((tiles, count), F32)], high, low)
    partner, own_partner = call(
        functools.partial(partner_kernel, scale), [((count, width), BF16), ((tiles, count), F32)], partner_rows, unit
    )
    high_rows, low, own_partner = lax.optimization_barrier((high_rows, low, own_partner))
    odd_rows = send(high_rows, odd)
    even_rows = send(low, even)
    far_of = lambda rows: call(
        functools.partial(far_kernel, scale),
        [((half, width), BF16), ((tiles // 2, count), F32), ((tiles, half), F32), ((tiles // 2, count), F32)],
        rows,
        unit,
        partner,
    )
    high_unit, own_high, high_own, partner_high = far_of(high_rows)
    low_unit, own_low, low_own, partner_low = far_of(low_rows)
    far_max, beside_max, cross_max, half_tiles = call(
        functools.partial(last_kernel, scale),
        [
            ((tiles + tiles // 2, count), F32),
            ((tiles, count), F32),
            ((tiles, half), F32),
            ((tiles // 2, count), F32),
        ],
        role,
        even_rows,
        odd_rows,
        unit,
        low_unit,
        high_unit,
        low_own,
        high_own,
        partner_low,
        partner_high,
        scratch=[pltpu.VMEM((half, width), BF16)],
    )
    cross_max = send(cross_max, cross)
    far_max = send(far_max, [(b, a) for a, b in far])
    beside_max = send(beside_max, beside)
    (out,) = call(
        join_kernel,
        [((OFFSETS * tiles, count), F32)],
        role,
        own,
        own_partner,
        own_low,
        own_high,
        half_tiles,
        far_max,
        beside_max,
        cross_max,
        last=True,
    )
    return jnp.transpose(out)


def solution(mesh):
    return jax.shard_map(
        body,
        mesh=mesh,
        in_specs=(P(AXES, None),),
        out_specs=P(AXES, None),
        check_vma=False,
    )
```

```python
import functools

import jax
import jax.numpy as jnp
from jax import lax
from jax.experimental import pallas as pl
from jax.experimental.pallas import tpu as pltpu
from jax.sharding import PartitionSpec as P


AXES = ("blk", "grp")
TILE = 128
STEP = 256
OFFSETS = 5
VMEM_LIMIT = 16 << 20
F32, BF16 = jnp.float32, jnp.bfloat16


def unit_of(rows):
    values = rows.astype(F32)
    mean = jnp.mean(values * values, axis=-1, keepdims=True)
    return (values * lax.rsqrt(mean + 1e-06)).astype(BF16)


def scores(left, right):
    return lax.dot_general(left, right, (((1,), (1,)), ((), ())), preferred_element_type=F32)


def best(scale, left, right, right_ref, right_at=0, left_ref=None, left_at=0, same=None):
    rows, keys = left.shape[0], right.shape[0]
    for m in range(0, rows, STEP):
        for n in range(0, keys, STEP):
            s = scores(left[m : m + STEP, :], right[n : n + STEP, :])
            if same is not None and m == n:
                s = jnp.where(same, -jnp.inf, s)
            tiles = jnp.max(s.reshape(STEP // TILE, TILE, STEP), axis=1)
            at = right_at + m // TILE
            right_ref[at : at + STEP // TILE, n : n + STEP] = tiles * scale
            if left_ref is not None:
                for t in range(STEP // TILE):
                    tile = jnp.max(s[:, t * TILE : (t + 1) * TILE], axis=1)
                    at = left_at + n // TILE + t
                    left_ref[at : at + 1, m : m + STEP] = tile.reshape(1, STEP) * scale


def place(role_ref):
    turn = lax.rem(role_ref[0], 4)
    step = lax.rem(lax.div(role_ref[0], 4), 2)
    return turn, step, jnp.logical_or(turn == 1, turn == 2)


def cut_kernel(at, rows_ref, cut_ref, sem):
    copy = pltpu.make_async_copy(rows_ref.at[at : at + cut_ref.shape[0], :], cut_ref, sem)
    copy.start()
    copy.wait()


def own_kernel(scale, high_ref, low_ref, unit_ref, own_ref):
    half = low_ref.shape[0]
    unit_ref[:half, :] = unit_of(low_ref[...])
    unit_ref[half:, :] = unit_of(high_ref[...])
    same = lax.broadcasted_iota(jnp.int32, (STEP, STEP), 0) == lax.broadcasted_iota(
        jnp.int32, (STEP, STEP), 1
    )
    best(scale, unit_ref, unit_ref, own_ref, same=same)


def partner_kernel(scale, rows_ref, unit_ref, partner_ref, max_ref):
    partner_ref[...] = unit_of(rows_ref[...])
    best(scale, partner_ref, unit_ref, max_ref)


def far_kernel(
    scale, rows_ref, unit_ref, partner_ref, far_ref, own_far_ref, far_own_ref, partner_far_ref
):
    far_ref[...] = unit_of(rows_ref[...])
    best(scale, far_ref, unit_ref, own_far_ref, left_ref=far_own_ref)
    best(scale, far_ref, partner_ref, partner_far_ref)


def low_kernel(
    scale, rows_ref, unit_ref, partner_ref, own_high_ref, high_own_ref, partner_high_ref,
    far_ref, own_far_ref, far_own_ref, partner_far_ref,
):
    half = rows_ref.shape[0]
    across = half // TILE
    far_kernel(scale, rows_ref, unit_ref, partner_ref, far_ref, own_far_ref, far_own_ref, partner_far_ref)
    own_far_ref[across:, :] = own_high_ref[...]
    far_own_ref[:, half:] = high_own_ref[...]
    partner_far_ref[across:, :] = partner_high_ref[...]


def last_kernel(
    scale, role_ref, even_ref, odd_ref, unit_ref, low_ref, high_ref, rows_ref, cross_ref, tiles_ref, half_ref
):
    _, step, middle = place(role_ref)
    half = half_ref.shape[0]
    across = half // TILE

    @pl.when(jnp.logical_and(step == 0, middle))
    def _():
        half_ref[...] = unit_of(even_ref[...])
        best(scale, half_ref, low_ref, cross_ref, left_ref=rows_ref)
        best(scale, half_ref, high_ref, cross_ref, right_at=across, left_ref=rows_ref, left_at=across)

    @pl.when(jnp.logical_and(step == 1, jnp.logical_not(middle)))
    def _():
        half_ref[...] = unit_of(odd_ref[...])
        best(scale, half_ref, unit_ref, tiles_ref, left_ref=cross_ref)


def join_kernel(
    role_ref, own_ref, own_partner_ref, own_far_ref, far_ref, beside_ref, tiles_ref, rows_ref, cross_ref, out_ref
):
    turn, step, middle = place(role_ref)
    tiles, _ = own_ref.shape
    across = tiles // 2

    def put(slots, *values):
        slot = slots[0]
        for i in range(1, 4):
            slot = jnp.where(turn == i, slots[i], slot)
        at = pl.multiple_of(slot * tiles, tiles)
        out_ref[pl.ds(at, tiles), :] = jnp.concatenate(values[1:], axis=values[0])

    put((2, 2, 2, 2), 0, own_ref[...])
    put((4, 4, 0, 0), 0, own_partner_ref[...])
    put((3, 0, 4, 1), 0, own_far_ref[...])
    put((0, 1, 3, 4), 0, far_ref[...])

    @pl.when(middle)
    def _():
        put((0, 3, 1, 0), 0, beside_ref[...])

    @pl.when(jnp.logical_and(jnp.logical_not(middle), step == 0))
    def _():
        put((1, 1, 1, 3), 1, rows_ref[...], cross_ref[...])

    @pl.when(jnp.logical_and(jnp.logical_not(middle), step == 1))
    def _():
        low = jnp.concatenate([cross_ref[:across, :], cross_ref[across:, :]], axis=1)
        put((1, 1, 1, 3), 0, low, tiles_ref[...])


def call(kernel, outs, *operands, scratch=(), source=False, last=False):
    specs, placed = [], []
    for value in operands:
        if value.dtype == jnp.int32:
            specs.append(pl.BlockSpec(memory_space=pltpu.SMEM))
            placed.append(value)
            continue
        space = pltpu.HBM if source else pltpu.VMEM
        specs.append(pl.BlockSpec(memory_space=space))
        placed.append(pltpu.with_memory_space_constraint(value, space))
    return pl.pallas_call(
        kernel,
        out_shape=[jax.ShapeDtypeStruct(*o) if last else pltpu.VMEM(*o) for o in outs],
        in_specs=specs,
        out_specs=[pl.BlockSpec(memory_space=pltpu.VMEM) for _ in outs],
        scratch_shapes=list(scratch),
        compiler_params=pltpu.CompilerParams(vmem_limit_bytes=VMEM_LIMIT),
    )(*placed)


def body(embeddings):
    count, width = embeddings.shape
    blocks = lax.axis_size(AXES[0]) * lax.axis_size(AXES[1])
    columns = blocks // 4
    assert blocks % 8 == 0 and count % (2 * STEP) == 0
    scale = 1.0 / width**0.5
    tiles, half = count // TILE, count // 2
    across = half // TILE

    at = lambda column, turn: column % columns * 4 + turn
    far, back, swap, even, odd, beside, rows, cross = [], [], [], [], [], [], [], []
    for q in range(columns):
        far += [(at(q, 1), at(q, 0)), (at(q, 2), at(q, 3))]
        far += [(at(q, 3), at(q + 1, 1)), (at(q, 0), at(q - 1, 2))]
        swap += [(at(q, 0), at(q, 2)), (at(q, 2), at(q, 0)), (at(q, 1), at(q, 3)), (at(q, 3), at(q, 1))]
        beside += [(at(q, 0), at(q, 2)), (at(q, 3), at(q, 1))]
        back += [(b, a) for a, b in far[-4:]]
        if q % 2 == 0:
            even += [(at(q, 0), at(q, 1)), (at(q, 3), at(q, 2))]
            rows += [(at(q, 1), at(q, 0)), (at(q, 2), at(q, 3))]
            cross += [(at(q, 1), at(q - 1, 3)), (at(q, 2), at(q + 1, 0))]
        else:
            odd += [(at(q, 1), at(q, 0)), (at(q, 2), at(q, 3))]
            cross += [(at(q, 0), at(q - 1, 3)), (at(q, 3), at(q + 1, 0))]

    def send(value, pairs):
        return lax.ppermute(value, AXES, pairs)

    role = lax.axis_index(AXES).astype(jnp.int32).reshape(1)
    role, embeddings = lax.optimization_barrier((role, embeddings))

    def cut(at):
        (part,) = call(
            functools.partial(cut_kernel, at),
            [((half, width), BF16)],
            embeddings,
            source=True,
            scratch=[pltpu.SemaphoreType.DMA],
        )
        return part

    high = cut(half)
    high_rows = send(high, far)
    high, embeddings = lax.optimization_barrier((high, embeddings))
    low = cut(0)
    low_rows = send(low, far)
    low, embeddings = lax.optimization_barrier((low, embeddings))
    partner_rows = send(embeddings, swap)
    unit, own = call(functools.partial(own_kernel, scale), [((count, width), BF16), ((tiles, count), F32)], high, low)
    partner, own_partner = call(
        functools.partial(partner_kernel, scale), [((count, width), BF16), ((tiles, count), F32)], partner_rows, unit
    )
    high_rows, own_partner = lax.optimization_barrier((high_rows, own_partner))
    odd_rows = send(high_rows, odd)
    high_unit, own_high, high_own, partner_high = call(
        functools.partial(far_kernel, scale),
        [((half, width), BF16), ((across, count), F32), ((tiles, half), F32), ((across, count), F32)],
        high_rows,
        unit,
        partner,
    )
    low, own_high = lax.optimization_barrier((low, own_high))
    even_rows = send(low, even)
    low_unit, own_far, far_own, partner_far = call(
        functools.partial(low_kernel, scale),
        [((half, width), BF16)] + [((tiles, count), F32)] * 3,
        low_rows,
        unit,
        partner,
        own_high,
        high_own,
        partner_high,
    )
    far_max = send(far_own, back)
    beside_max = send(partner_far, beside)
    rows_max, cross_max, half_tiles = call(
        functools.partial(last_kernel, scale),
        [((tiles, half), F32), ((tiles, half), F32), ((across, count), F32)],
        role,
        even_rows,
        odd_rows,
        unit,
        low_unit,
        high_unit,
        scratch=[pltpu.VMEM((half, width), BF16)],
    )
    rows_max = send(rows_max, rows)
    cross_max = send(cross_max, cross)
    (out,) = call(
        join_kernel,
        [((OFFSETS * tiles, count), F32)],
        role,
        own,
        own_partner,
        own_far,
        far_max,
        beside_max,
        half_tiles,
        rows_max,
        cross_max,
        last=True,
    )
    return jnp.transpose(out)


def solution(mesh):
    return jax.shard_map(
        body,
        mesh=mesh,
        in_specs=(P(AXES, None),),
        out_specs=P(AXES, None),
        check_vma=False,
    )
```

```python
import functools

import jax
import jax.numpy as jnp
from jax import lax
from jax.experimental import pallas as pl
from jax.experimental.pallas import tpu as pltpu
from jax.sharding import PartitionSpec as P


AXES = ("blk", "grp")
TILE = 128
STEP = 256
PARTS = 2
OFFSETS = 5
VMEM_LIMIT = 16 << 20
F32, BF16 = jnp.float32, jnp.bfloat16


def unit_of(rows):
    values = rows.astype(F32)
    mean = jnp.mean(values * values, axis=-1, keepdims=True)
    return (values * lax.rsqrt(mean + 1e-06)).astype(BF16)


def scores(left, right):
    return lax.dot_general(left, right, (((1,), (1,)), ((), ())), preferred_element_type=F32)


def best(scale, left, right, right_ref, right_at=0, left_ref=None, left_at=0, left_from=0, same=None):
    rows, keys = left.shape[0], right.shape[0]
    for m in range(0, rows, STEP):
        for n in range(0, keys, STEP):
            s = scores(left[m : m + STEP, :], right[n : n + STEP, :])
            if same is not None and m == n:
                s = jnp.where(same, -jnp.inf, s)
            tiles = jnp.max(s.reshape(STEP // TILE, TILE, STEP), axis=1)
            at = right_at + m // TILE
            right_ref[at : at + STEP // TILE, n : n + STEP] = tiles * scale
            if left_ref is not None:
                for t in range(STEP // TILE):
                    tile = jnp.max(s[:, t * TILE : (t + 1) * TILE], axis=1)
                    at = left_at + n // TILE + t
                    left_ref[at : at + 1, left_from + m : left_from + m + STEP] = tile.reshape(1, STEP) * scale


def place(role_ref):
    turn = lax.rem(role_ref[0], 4)
    step = lax.rem(lax.div(role_ref[0], 4), 2)
    return turn, step, jnp.logical_or(turn == 1, turn == 2)


def own_kernel(scale, rows_ref, unit_ref, own_ref):
    unit_ref[...] = unit_of(rows_ref[...])
    same = lax.broadcasted_iota(jnp.int32, (STEP, STEP), 0) == lax.broadcasted_iota(
        jnp.int32, (STEP, STEP), 1
    )
    best(scale, unit_ref, unit_ref, own_ref, same=same)


def partner_kernel(role_ref, rows_ref, unit_ref, partner_ref, *part_refs):
    middle = place(role_ref)[2]
    size = part_refs[0].shape[0]
    half = size * len(part_refs)
    partner_ref[...] = unit_of(rows_ref[...])
    for i, part_ref in enumerate(part_refs):
        at = i * size

        @pl.when(middle)
        def _():
            part_ref[...] = partner_ref[at : at + size, :]

        @pl.when(jnp.logical_not(middle))
        def _():
            part_ref[...] = unit_ref[half + at : half + at + size, :]


def pair_kernel(scale, unit_ref, partner_ref, max_ref):
    best(scale, partner_ref, unit_ref, max_ref)


def far_kernel(scale, role_ref, rows_ref, unit_ref, partner_ref, far_ref, own_far_ref, far_max_ref):
    middle = place(role_ref)[2]
    tiles = own_far_ref.shape[0]
    far_ref[...] = unit_of(rows_ref[...])
    best(scale, far_ref, unit_ref, own_far_ref, left_ref=far_max_ref)

    @pl.when(jnp.logical_not(middle))
    def _():
        best(scale, partner_ref, far_ref, far_max_ref, right_at=tiles)


def part_kernel(scale, first, role_ref, part_ref, unit_ref, far_ref, *refs):
    _, step, middle = place(role_ref)
    rows_ref, cross_ref, tiles_ref = refs[-3:]
    count = unit_ref.shape[0]
    half, across = count // 2, count // 2 // TILE
    inside = jnp.logical_and(step == 0, middle)
    outside = jnp.logical_and(step == 1, jnp.logical_not(middle))
    at = first // TILE

    if first:
        old_rows_ref, old_cross_ref, old_tiles_ref = refs[:3]

        @pl.when(inside)
        def _():
            rows_ref[:, :first] = old_rows_ref[:, :first]
            cross_ref[:at, :] = old_cross_ref[:at, :]
            cross_ref[across : across + at, :] = old_cross_ref[across : across + at, :]

        @pl.when(outside)
        def _():
            cross_ref[:, :first] = old_cross_ref[:, :first]
            tiles_ref[:at, :] = old_tiles_ref[:at, :]

    @pl.when(inside)
    def _():
        best(scale, part_ref, far_ref.at[:half, :], cross_ref, right_at=at, left_ref=rows_ref, left_from=first)
        best(
            scale, part_ref, far_ref.at[half:, :], cross_ref, right_at=across + at,
            left_ref=rows_ref, left_at=across, left_from=first,
        )

    @pl.when(outside)
    def _():
        best(scale, part_ref, unit_ref, tiles_ref, right_at=at, left_ref=cross_ref, left_from=first)


def join_kernel(
    role_ref, own_ref, own_partner_ref, own_far_ref, far_ref, tiles_ref, rows_ref, cross_ref, out_ref
):
    turn, step, middle = place(role_ref)
    tiles, _ = own_ref.shape
    across = tiles // 2

    def put(slots, *values):
        slot = slots[0]
        for i in range(1, 4):
            slot = jnp.where(turn == i, slots[i], slot)
        at = pl.multiple_of(slot * tiles, tiles)
        out_ref[pl.ds(at, tiles), :] = jnp.concatenate(values[1:], axis=values[0])

    put((2, 2, 2, 2), 0, own_ref[...])
    put((4, 4, 0, 0), 0, own_partner_ref[...])
    put((3, 0, 4, 1), 0, own_far_ref[...])
    put((0, 1, 3, 4), 0, far_ref[:tiles, :])

    @pl.when(middle)
    def _():
        put((0, 3, 1, 0), 0, far_ref[tiles:, :])

    @pl.when(jnp.logical_and(jnp.logical_not(middle), step == 0))
    def _():
        put((1, 1, 1, 3), 1, rows_ref[...], cross_ref[...])

    @pl.when(jnp.logical_and(jnp.logical_not(middle), step == 1))
    def _():
        low = jnp.concatenate([cross_ref[:across, :], cross_ref[across:, :]], axis=1)
        put((1, 1, 1, 3), 0, low, tiles_ref[...])


def call(kernel, outs, *operands, last=False):
    specs, placed = [], []
    for value in operands:
        scalar = value.dtype == jnp.int32
        specs.append(pl.BlockSpec(memory_space=pltpu.SMEM if scalar else pltpu.VMEM))
        placed.append(value if scalar else pltpu.with_memory_space_constraint(value, pltpu.VMEM))
    return pl.pallas_call(
        kernel,
        out_shape=[jax.ShapeDtypeStruct(*o) if last else pltpu.VMEM(*o) for o in outs],
        in_specs=specs,
        out_specs=[pl.BlockSpec(memory_space=pltpu.VMEM) for _ in outs],
        compiler_params=pltpu.CompilerParams(vmem_limit_bytes=VMEM_LIMIT),
    )(*placed)


def body(embeddings):
    count, width = embeddings.shape
    blocks = lax.axis_size(AXES[0]) * lax.axis_size(AXES[1])
    columns = blocks // 4
    scale = 1.0 / width**0.5
    tiles, half = count // TILE, count // 2
    across, size = half // TILE, half // PARTS
    assert blocks % 8 == 0 and size % STEP == 0

    at = lambda column, turn: column % columns * 4 + turn
    far, swap, parts, rows, cross = [], [], [], [], []
    for q in range(columns):
        far += [(at(q, 1), at(q, 0)), (at(q, 2), at(q, 3))]
        far += [(at(q, 3), at(q + 1, 1)), (at(q, 0), at(q - 1, 2))]
        swap += [(at(q, 0), at(q, 2)), (at(q, 2), at(q, 0)), (at(q, 1), at(q, 3)), (at(q, 3), at(q, 1))]
        if q % 2 == 0:
            parts += [(at(q, 1), at(q, 2)), (at(q, 2), at(q, 1))]
            parts += [(at(q, 3), at(q + 1, 0)), (at(q, 0), at(q - 1, 3))]
            rows += [(at(q, 1), at(q, 0)), (at(q, 2), at(q, 3))]
            cross += [(at(q, 1), at(q - 1, 3)), (at(q, 2), at(q + 1, 0))]
        else:
            cross += [(at(q, 0), at(q - 1, 3)), (at(q, 3), at(q + 1, 0))]

    def send(value, pairs):
        return lax.ppermute(value, AXES, pairs)

    role = lax.axis_index(AXES).astype(jnp.int32).reshape(1)
    role, embeddings = lax.optimization_barrier((role, embeddings))
    far_rows = send(embeddings, far)
    partner_rows = send(embeddings, swap)
    unit, own = call(functools.partial(own_kernel, scale), [((count, width), BF16), ((tiles, count), F32)], embeddings)
    partner, *pieces = call(
        partner_kernel, [((count, width), BF16)] + [((size, width), BF16)] * PARTS, role, partner_rows, unit
    )
    pieces = [send(piece, parts) for piece in pieces]
    (own_partner,) = call(functools.partial(pair_kernel, scale), [((tiles, count), F32)], unit, partner)
    far_unit, own_far, far_max = call(
        functools.partial(far_kernel, scale),
        [((count, width), BF16), ((tiles, count), F32), ((2 * tiles, count), F32)],
        role,
        far_rows,
        unit,
        partner,
    )
    far_max = send(far_max, [(b, a) for a, b in far])
    done = []
    for i, piece in enumerate(pieces):
        done = call(
            functools.partial(part_kernel, scale, i * size),
            [((tiles, half), F32), ((tiles, half), F32), ((across, count), F32)],
            role,
            piece,
            unit,
            far_unit,
            *done,
        )
    rows_max, cross_max, half_tiles = done
    rows_max = send(rows_max, rows)
    cross_max = send(cross_max, cross)
    (out,) = call(
        join_kernel,
        [((OFFSETS * tiles, count), F32)],
        role,
        own,
        own_partner,
        own_far,
        far_max,
        half_tiles,
        rows_max,
        cross_max,
        last=True,
    )
    return jnp.transpose(out)


def solution(mesh):
    return jax.shard_map(
        body,
        mesh=mesh,
        in_specs=(P(AXES, None),),
        out_specs=P(AXES, None),
        check_vma=False,
    )
```

```python
import functools

import jax
import jax.numpy as jnp
from jax import lax
from jax.experimental import pallas as pl
from jax.experimental.pallas import tpu as pltpu
from jax.sharding import PartitionSpec as P


AXES = ("blk", "grp")
TILE = 128
STEP = 256
PARTS = 2
OFFSETS = 5
VMEM_LIMIT = 16 << 20
F32, BF16 = jnp.float32, jnp.bfloat16


def unit_of(rows):
    values = rows.astype(F32)
    mean = jnp.mean(values * values, axis=-1, keepdims=True)
    return (values * lax.rsqrt(mean + 1e-06)).astype(BF16)


def scores(left, right):
    return lax.dot_general(left, right, (((1,), (1,)), ((), ())), preferred_element_type=F32)


def best(scale, left, right, right_ref, right_at=0, left_ref=None, left_at=0, left_from=0, same=None):
    rows, keys = left.shape[0], right.shape[0]
    for m in range(0, rows, STEP):
        for n in range(0, keys, STEP):
            s = scores(left[m : m + STEP, :], right[n : n + STEP, :])
            if same is not None and m == n:
                s = jnp.where(same, -jnp.inf, s)
            tiles = jnp.max(s.reshape(STEP // TILE, TILE, STEP), axis=1)
            at = right_at + m // TILE
            right_ref[at : at + STEP // TILE, n : n + STEP] = tiles * scale
            if left_ref is not None:
                for t in range(STEP // TILE):
                    tile = jnp.max(s[:, t * TILE : (t + 1) * TILE], axis=1)
                    at = left_at + n // TILE + t
                    left_ref[at : at + 1, left_from + m : left_from + m + STEP] = tile.reshape(1, STEP) * scale


def place(role_ref):
    turn = lax.rem(role_ref[0], 4)
    step = lax.rem(lax.div(role_ref[0], 4), 2)
    return turn, step, jnp.logical_or(turn == 1, turn == 2)


def own_kernel(scale, rows_ref, unit_ref, own_ref):
    unit_ref[...] = unit_of(rows_ref[...])
    same = lax.broadcasted_iota(jnp.int32, (STEP, STEP), 0) == lax.broadcasted_iota(
        jnp.int32, (STEP, STEP), 1
    )
    best(scale, unit_ref, unit_ref, own_ref, same=same)


def partner_kernel(role_ref, rows_ref, unit_ref, partner_ref, *part_refs):
    middle = place(role_ref)[2]
    size = part_refs[0].shape[0]
    half = size * len(part_refs)
    partner_ref[...] = unit_of(rows_ref[...])
    for i, part_ref in enumerate(part_refs):
        at = i * size

        @pl.when(middle)
        def _():
            part_ref[...] = partner_ref[at : at + size, :]

        @pl.when(jnp.logical_not(middle))
        def _():
            part_ref[...] = unit_ref[half + at : half + at + size, :]


def pair_kernel(scale, unit_ref, partner_ref, max_ref):
    best(scale, partner_ref, unit_ref, max_ref)


def far_kernel(scale, role_ref, rows_ref, unit_ref, partner_ref, far_ref, own_far_ref, far_max_ref):
    middle = place(role_ref)[2]
    tiles = own_far_ref.shape[0]
    far_ref[...] = unit_of(rows_ref[...])
    best(scale, far_ref, unit_ref, own_far_ref, left_ref=far_max_ref)

    @pl.when(jnp.logical_not(middle))
    def _():
        best(scale, partner_ref, far_ref, far_max_ref, right_at=tiles)


def part_kernel(scale, first, role_ref, part_ref, unit_ref, far_ref, *refs):
    _, step, middle = place(role_ref)
    rows_ref, cross_ref, tiles_ref = refs[-3:]
    count = unit_ref.shape[0]
    half, across = count // 2, count // 2 // TILE
    inside = jnp.logical_and(step == 0, middle)
    outside = jnp.logical_and(step == 1, jnp.logical_not(middle))
    at = first // TILE

    if first:
        old_rows_ref, old_cross_ref, old_tiles_ref = refs[:3]

        @pl.when(inside)
        def _():
            rows_ref[:, :first] = old_rows_ref[:, :first]
            cross_ref[:at, :] = old_cross_ref[:at, :]
            cross_ref[across : across + at, :] = old_cross_ref[across : across + at, :]

        @pl.when(outside)
        def _():
            cross_ref[:, :first] = old_cross_ref[:, :first]
            tiles_ref[:at, :] = old_tiles_ref[:at, :]

    @pl.when(inside)
    def _():
        best(scale, part_ref, far_ref.at[:half, :], cross_ref, right_at=at, left_ref=rows_ref, left_from=first)
        best(
            scale, part_ref, far_ref.at[half:, :], cross_ref, right_at=across + at,
            left_ref=rows_ref, left_at=across, left_from=first,
        )

    @pl.when(outside)
    def _():
        best(scale, part_ref, unit_ref, tiles_ref, right_at=at, left_ref=cross_ref, left_from=first)


def join_kernel(
    role_ref, own_ref, own_partner_ref, own_far_ref, far_ref, tiles_ref, rows_ref, cross_ref, ends_ref, out_ref
):
    turn, step, middle = place(role_ref)
    tiles, _ = own_ref.shape
    across = tiles // 2

    def put(slots, *values):
        slot = slots[0]
        for i in range(1, 4):
            slot = jnp.where(turn == i, slots[i], slot)
        at = pl.multiple_of(slot * tiles, tiles)
        out_ref[pl.ds(at, tiles), :] = jnp.concatenate(values[1:], axis=values[0])

    put((2, 2, 2, 2), 0, own_ref[...])
    put((4, 4, 0, 0), 0, own_partner_ref[...])
    put((3, 0, 4, 1), 0, own_far_ref[...])
    put((0, 1, 3, 4), 0, far_ref[:tiles, :])

    @pl.when(middle)
    def _():
        put((0, 3, 1, 0), 0, far_ref[tiles:, :])

    @pl.when(jnp.logical_and(jnp.logical_not(middle), step == 0))
    def _():
        put((1, 1, 1, 3), 1, rows_ref[...], cross_ref[...])

    @pl.when(jnp.logical_and(jnp.logical_not(middle), step == 1))
    def _():
        low = jnp.concatenate([ends_ref[:across, :], ends_ref[across:, :]], axis=1)
        put((1, 1, 1, 3), 0, low, tiles_ref[...])


def call(kernel, outs, *operands, last=False):
    specs, placed = [], []
    for value in operands:
        scalar = value.dtype == jnp.int32
        specs.append(pl.BlockSpec(memory_space=pltpu.SMEM if scalar else pltpu.VMEM))
        placed.append(value if scalar else pltpu.with_memory_space_constraint(value, pltpu.VMEM))
    return pl.pallas_call(
        kernel,
        out_shape=[jax.ShapeDtypeStruct(*o) if last else pltpu.VMEM(*o) for o in outs],
        in_specs=specs,
        out_specs=[pl.BlockSpec(memory_space=pltpu.VMEM) for _ in outs],
        compiler_params=pltpu.CompilerParams(vmem_limit_bytes=VMEM_LIMIT),
    )(*placed)


def body(embeddings):
    count, width = embeddings.shape
    blocks = lax.axis_size(AXES[0]) * lax.axis_size(AXES[1])
    columns = blocks // 4
    scale = 1.0 / width**0.5
    tiles, half = count // TILE, count // 2
    across, size = half // TILE, half // PARTS
    assert blocks % 8 == 0 and size % STEP == 0

    at = lambda column, turn: column % columns * 4 + turn
    far, swap, parts, rows, cross, ends = [], [], [], [], [], []
    for q in range(columns):
        far += [(at(q, 1), at(q, 0)), (at(q, 2), at(q, 3))]
        far += [(at(q, 3), at(q + 1, 1)), (at(q, 0), at(q - 1, 2))]
        swap += [(at(q, 0), at(q, 2)), (at(q, 2), at(q, 0)), (at(q, 1), at(q, 3)), (at(q, 3), at(q, 1))]
        if q % 2 == 0:
            parts += [(at(q, 1), at(q, 2)), (at(q, 2), at(q, 1))]
            parts += [(at(q, 3), at(q + 1, 0)), (at(q, 0), at(q - 1, 3))]
            rows += [(at(q, 1), at(q, 0)), (at(q, 2), at(q, 3))]
            ends += [(at(q, 1), at(q - 1, 3)), (at(q, 2), at(q + 1, 0))]
        else:
            cross += [(at(q, 0), at(q - 1, 3)), (at(q, 3), at(q + 1, 0))]

    def send(value, pairs):
        return lax.ppermute(value, AXES, pairs)

    role = lax.axis_index(AXES).astype(jnp.int32).reshape(1)
    role, embeddings = lax.optimization_barrier((role, embeddings))
    far_rows = send(embeddings, far)
    partner_rows = send(embeddings, swap)
    unit, own = call(functools.partial(own_kernel, scale), [((count, width), BF16), ((tiles, count), F32)], embeddings)
    partner, *pieces = call(
        partner_kernel, [((count, width), BF16)] + [((size, width), BF16)] * PARTS, role, partner_rows, unit
    )
    pieces = [send(piece, parts) for piece in pieces]
    (own_partner,) = call(functools.partial(pair_kernel, scale), [((tiles, count), F32)], unit, partner)
    far_unit, own_far, far_max = call(
        functools.partial(far_kernel, scale),
        [((count, width), BF16), ((tiles, count), F32), ((2 * tiles, count), F32)],
        role,
        far_rows,
        unit,
        partner,
    )
    far_max = send(far_max, [(b, a) for a, b in far])
    done = []
    for i, piece in enumerate(pieces):
        done = call(
            functools.partial(part_kernel, scale, i * size),
            [((tiles, half), F32), ((tiles, half), F32), ((across, count), F32)],
            role,
            piece,
            unit,
            far_unit,
            *done,
        )
    rows_max, cross_max, half_tiles = done
    ends_max = send(cross_max, ends)
    rows_max = send(rows_max, rows)
    cross_max = send(cross_max, cross)
    (out,) = call(
        join_kernel,
        [((OFFSETS * tiles, count), F32)],
        role,
        own,
        own_partner,
        own_far,
        far_max,
        half_tiles,
        rows_max,
        cross_max,
        ends_max,
        last=True,
    )
    return jnp.transpose(out)


def solution(mesh):
    return jax.shard_map(
        body,
        mesh=mesh,
        in_specs=(P(AXES, None),),
        out_specs=P(AXES, None),
        check_vma=False,
    )
```

```python
import functools

import jax
import jax.numpy as jnp
from jax import lax
from jax.experimental import pallas as pl
from jax.experimental.pallas import tpu as pltpu
from jax.sharding import PartitionSpec as P


AXES = ("blk", "grp")
TILE = 128
STEP = 256
PARTS = 2
OFFSETS = 5
VMEM_LIMIT = 16 << 20
F32, BF16 = jnp.float32, jnp.bfloat16


def unit_of(rows):
    values = rows.astype(F32)
    mean = jnp.mean(values * values, axis=-1, keepdims=True)
    return (values * lax.rsqrt(mean + 1e-06)).astype(BF16)


def scores(left, right):
    return lax.dot_general(left, right, (((1,), (1,)), ((), ())), preferred_element_type=F32)


def best(scale, left, right, right_ref, right_at=0, left_ref=None, left_at=0, left_from=0, same=None):
    rows, keys = left.shape[0], right.shape[0]
    for m in range(0, rows, STEP):
        for n in range(0, keys, STEP):
            s = scores(left[m : m + STEP, :], right[n : n + STEP, :])
            if same is not None and m == n:
                s = jnp.where(same, -jnp.inf, s)
            tiles = jnp.max(s.reshape(STEP // TILE, TILE, STEP), axis=1)
            at = right_at + m // TILE
            right_ref[at : at + STEP // TILE, n : n + STEP] = tiles * scale
            if left_ref is not None:
                for t in range(STEP // TILE):
                    tile = jnp.max(s[:, t * TILE : (t + 1) * TILE], axis=1)
                    at = left_at + n // TILE + t
                    left_ref[at : at + 1, left_from + m : left_from + m + STEP] = tile.reshape(1, STEP) * scale


def place(role_ref):
    turn = lax.rem(role_ref[0], 4)
    step = lax.rem(lax.div(role_ref[0], 4), 2)
    return turn, step, jnp.logical_or(turn == 1, turn == 2)


def own_kernel(scale, rows_ref, unit_ref, own_ref, *part_refs):
    unit_ref[...] = unit_of(rows_ref[...])
    size = part_refs[0].shape[0]
    for i, part_ref in enumerate(part_refs):
        at = (len(part_refs) + i) * size
        part_ref[...] = unit_ref[at : at + size, :]
    same = lax.broadcasted_iota(jnp.int32, (STEP, STEP), 0) == lax.broadcasted_iota(
        jnp.int32, (STEP, STEP), 1
    )
    best(scale, unit_ref, unit_ref, own_ref, same=same)


def partner_kernel(rows_ref, partner_ref, *part_refs):
    partner_ref[...] = unit_of(rows_ref[...])
    size = part_refs[0].shape[0]
    for i, part_ref in enumerate(part_refs):
        part_ref[...] = partner_ref[i * size : (i + 1) * size, :]


def pair_kernel(scale, unit_ref, partner_ref, max_ref):
    best(scale, partner_ref, unit_ref, max_ref)


def far_kernel(scale, role_ref, rows_ref, unit_ref, partner_ref, far_ref, own_far_ref, far_max_ref):
    middle = place(role_ref)[2]
    tiles = own_far_ref.shape[0]
    far_ref[...] = unit_of(rows_ref[...])
    best(scale, far_ref, unit_ref, own_far_ref, left_ref=far_max_ref)

    @pl.when(jnp.logical_not(middle))
    def _():
        best(scale, partner_ref, far_ref, far_max_ref, right_at=tiles)


def even_kernel(first, scale, role_ref, part_ref, far_ref, *refs):
    _, step, middle = place(role_ref)
    rows_ref, ends_ref = refs[-2:]
    half = far_ref.shape[0] // 2
    at, across = first // TILE, half // TILE

    @pl.when(jnp.logical_and(step == 0, middle))
    def _():
        if first:
            old_rows_ref, old_ends_ref = refs[:2]
            rows_ref[:, :first] = old_rows_ref[:, :first]
            ends_ref[:at, :] = old_ends_ref[:at, :]
            ends_ref[across : across + at, :] = old_ends_ref[across : across + at, :]
        best(scale, part_ref, far_ref.at[:half, :], ends_ref, right_at=at, left_ref=rows_ref, left_from=first)
        best(
            scale, part_ref, far_ref.at[half:, :], ends_ref, right_at=across + at,
            left_ref=rows_ref, left_at=across, left_from=first,
        )


def odd_kernel(first, scale, role_ref, part_ref, unit_ref, *refs):
    _, step, middle = place(role_ref)
    cross_ref, tiles_ref = refs[-2:]
    at = first // TILE

    @pl.when(jnp.logical_and(step == 1, jnp.logical_not(middle)))
    def _():
        if first:
            old_cross_ref, old_tiles_ref = refs[:2]
            cross_ref[:, :first] = old_cross_ref[:, :first]
            tiles_ref[:at, :] = old_tiles_ref[:at, :]
        best(scale, part_ref, unit_ref, tiles_ref, right_at=at, left_ref=cross_ref, left_from=first)


def join_kernel(
    role_ref, own_ref, own_partner_ref, own_far_ref, far_ref, tiles_ref, rows_ref, cross_ref, ends_ref, out_ref
):
    turn, step, middle = place(role_ref)
    tiles, _ = own_ref.shape
    across = tiles // 2

    def put(slots, *values):
        slot = slots[0]
        for i in range(1, 4):
            slot = jnp.where(turn == i, slots[i], slot)
        at = pl.multiple_of(slot * tiles, tiles)
        out_ref[pl.ds(at, tiles), :] = jnp.concatenate(values[1:], axis=values[0])

    put((2, 2, 2, 2), 0, own_ref[...])
    put((4, 4, 0, 0), 0, own_partner_ref[...])
    put((3, 0, 4, 1), 0, own_far_ref[...])
    put((0, 1, 3, 4), 0, far_ref[:tiles, :])

    @pl.when(middle)
    def _():
        put((0, 3, 1, 0), 0, far_ref[tiles:, :])

    @pl.when(jnp.logical_and(jnp.logical_not(middle), step == 0))
    def _():
        put((1, 1, 1, 3), 1, rows_ref[...], cross_ref[...])

    @pl.when(jnp.logical_and(jnp.logical_not(middle), step == 1))
    def _():
        low = jnp.concatenate([ends_ref[:across, :], ends_ref[across:, :]], axis=1)
        put((1, 1, 1, 3), 0, low, tiles_ref[...])


def call(kernel, outs, *operands, last=False):
    specs, placed = [], []
    for value in operands:
        scalar = value.dtype == jnp.int32
        specs.append(pl.BlockSpec(memory_space=pltpu.SMEM if scalar else pltpu.VMEM))
        placed.append(value if scalar else pltpu.with_memory_space_constraint(value, pltpu.VMEM))
    return pl.pallas_call(
        kernel,
        out_shape=[jax.ShapeDtypeStruct(*o) if last else pltpu.VMEM(*o) for o in outs],
        in_specs=specs,
        out_specs=[pl.BlockSpec(memory_space=pltpu.VMEM) for _ in outs],
        compiler_params=pltpu.CompilerParams(vmem_limit_bytes=VMEM_LIMIT),
    )(*placed)


def body(embeddings):
    count, width = embeddings.shape
    blocks = lax.axis_size(AXES[0]) * lax.axis_size(AXES[1])
    columns = blocks // 4
    scale = 1.0 / width**0.5
    tiles, half = count // TILE, count // 2
    across, size = half // TILE, half // PARTS
    assert blocks % 8 == 0 and size % STEP == 0

    at = lambda column, turn: column % columns * 4 + turn
    far, swap, even, odd, rows, cross, ends = [], [], [], [], [], [], []
    for q in range(columns):
        far += [(at(q, 1), at(q, 0)), (at(q, 2), at(q, 3))]
        far += [(at(q, 3), at(q + 1, 1)), (at(q, 0), at(q - 1, 2))]
        swap += [(at(q, 0), at(q, 2)), (at(q, 2), at(q, 0)), (at(q, 1), at(q, 3)), (at(q, 3), at(q, 1))]
        if q % 2 == 0:
            even += [(at(q, 1), at(q, 2)), (at(q, 2), at(q, 1))]
            odd += [(at(q, 3), at(q + 1, 0)), (at(q, 0), at(q - 1, 3))]
            rows += [(at(q, 1), at(q, 0)), (at(q, 2), at(q, 3))]
            ends += [(at(q, 1), at(q - 1, 3)), (at(q, 2), at(q + 1, 0))]
        else:
            cross += [(at(q, 0), at(q - 1, 3)), (at(q, 3), at(q + 1, 0))]

    def send(value, pairs):
        return lax.ppermute(value, AXES, pairs)

    role = lax.axis_index(AXES).astype(jnp.int32).reshape(1)
    role, embeddings = lax.optimization_barrier((role, embeddings))
    far_rows = send(embeddings, far)
    partner_rows = send(embeddings, swap)
    piece = ((size, width), BF16)
    unit, own, *odd_parts = call(
        functools.partial(own_kernel, scale),
        [((count, width), BF16), ((tiles, count), F32)] + [piece] * PARTS,
        embeddings,
    )
    odd_parts = [send(part, odd) for part in odd_parts]
    partner, *even_parts = call(partner_kernel, [((count, width), BF16)] + [piece] * PARTS, partner_rows)
    even_parts = [send(part, even) for part in even_parts]
    (own_partner,) = call(functools.partial(pair_kernel, scale), [((tiles, count), F32)], unit, partner)
    far_unit, own_far, far_max = call(
        functools.partial(far_kernel, scale),
        [((count, width), BF16), ((tiles, count), F32), ((2 * tiles, count), F32)],
        role,
        far_rows,
        unit,
        partner,
    )
    far_max = send(far_max, [(b, a) for a, b in far])
    column = ((tiles, half), F32)
    done = []
    for i, part in enumerate(even_parts):
        done = call(functools.partial(even_kernel, i * size, scale), [column, column], role, part, far_unit, *done)
    rows_max, ends_max = done
    ends_max = send(ends_max, ends)
    rows_max = send(rows_max, rows)
    done = []
    for i, part in enumerate(odd_parts):
        done = call(
            functools.partial(odd_kernel, i * size, scale), [column, ((across, count), F32)], role, part, unit, *done
        )
    cross_max, half_tiles = done
    cross_max = send(cross_max, cross)
    (out,) = call(
        join_kernel,
        [((OFFSETS * tiles, count), F32)],
        role,
        own,
        own_partner,
        own_far,
        far_max,
        half_tiles,
        rows_max,
        cross_max,
        ends_max,
        last=True,
    )
    return jnp.transpose(out)


def solution(mesh):
    return jax.shard_map(
        body,
        mesh=mesh,
        in_specs=(P(AXES, None),),
        out_specs=P(AXES, None),
        check_vma=False,
    )
```

```python
import functools

import jax
import jax.numpy as jnp
from jax import lax
from jax.experimental import pallas as pl
from jax.experimental.pallas import tpu as pltpu
from jax.sharding import PartitionSpec as P


AXES = ("blk", "grp")
TILE = 128
STEP = 256
PARTS = 2
OFFSETS = 5
VMEM_LIMIT = 16 << 20
F32, BF16 = jnp.float32, jnp.bfloat16


def unit_of(rows):
    values = rows.astype(F32)
    mean = jnp.mean(values * values, axis=-1, keepdims=True)
    return (values * lax.rsqrt(mean + 1e-06)).astype(BF16)


def scores(left, right):
    return lax.dot_general(left, right, (((1,), (1,)), ((), ())), preferred_element_type=F32)


def best(scale, left, right, right_ref, right_at=0, left_ref=None, left_at=0, left_from=0, same=None):
    rows, keys = left.shape[0], right.shape[0]
    for m in range(0, rows, STEP):
        for n in range(0, keys, STEP):
            s = scores(left[m : m + STEP, :], right[n : n + STEP, :])
            if same is not None and m == n:
                s = jnp.where(same, -jnp.inf, s)
            tiles = jnp.max(s.reshape(STEP // TILE, TILE, STEP), axis=1)
            at = right_at + m // TILE
            right_ref[at : at + STEP // TILE, n : n + STEP] = tiles * scale
            if left_ref is not None:
                for t in range(STEP // TILE):
                    tile = jnp.max(s[:, t * TILE : (t + 1) * TILE], axis=1)
                    at = left_at + n // TILE + t
                    left_ref[at : at + 1, left_from + m : left_from + m + STEP] = tile.reshape(1, STEP) * scale


def place(role_ref):
    turn = lax.rem(role_ref[0], 4)
    step = lax.rem(lax.div(role_ref[0], 4), 2)
    return turn, step, jnp.logical_or(turn == 1, turn == 2)


def own_kernel(scale, rows_ref, unit_ref, own_ref, *part_refs):
    unit_ref[...] = unit_of(rows_ref[...])
    size = part_refs[0].shape[0]
    for i, part_ref in enumerate(part_refs):
        at = (len(part_refs) + i) * size
        part_ref[...] = unit_ref[at : at + size, :]
    same = lax.broadcasted_iota(jnp.int32, (STEP, STEP), 0) == lax.broadcasted_iota(
        jnp.int32, (STEP, STEP), 1
    )
    best(scale, unit_ref, unit_ref, own_ref, same=same)


def partner_kernel(rows_ref, partner_ref, *part_refs):
    partner_ref[...] = unit_of(rows_ref[...])
    size = part_refs[0].shape[0]
    for i, part_ref in enumerate(part_refs):
        part_ref[...] = partner_ref[i * size : (i + 1) * size, :]


def pair_kernel(scale, unit_ref, partner_ref, max_ref):
    best(scale, partner_ref, unit_ref, max_ref)


def far_kernel(scale, role_ref, rows_ref, unit_ref, partner_ref, far_ref, own_far_ref, far_max_ref):
    middle = place(role_ref)[2]
    tiles = own_far_ref.shape[0]
    far_ref[...] = unit_of(rows_ref[...])
    best(scale, far_ref, unit_ref, own_far_ref, left_ref=far_max_ref)

    @pl.when(jnp.logical_not(middle))
    def _():
        best(scale, partner_ref, far_ref, far_max_ref, right_at=tiles)


def even_kernel(first, scale, role_ref, part_ref, far_ref, *refs):
    _, step, middle = place(role_ref)
    rows_ref, ends_ref = refs[-2:]
    half = far_ref.shape[0] // 2
    at, across = first // TILE, half // TILE

    @pl.when(jnp.logical_and(step == 0, middle))
    def _():
        if first:
            old_rows_ref, old_ends_ref = refs[:2]
            rows_ref[:, :first] = old_rows_ref[:, :first]
            ends_ref[:at, :] = old_ends_ref[:at, :]
            ends_ref[across : across + at, :] = old_ends_ref[across : across + at, :]
        best(scale, part_ref, far_ref.at[:half, :], ends_ref, right_at=at, left_ref=rows_ref, left_from=first)
        best(
            scale, part_ref, far_ref.at[half:, :], ends_ref, right_at=across + at,
            left_ref=rows_ref, left_at=across, left_from=first,
        )


def odd_kernel(first, scale, role_ref, part_ref, unit_ref, *refs):
    _, step, middle = place(role_ref)
    cross_ref, tiles_ref = refs[-2:]
    at = first // TILE

    @pl.when(jnp.logical_and(step == 1, jnp.logical_not(middle)))
    def _():
        if first:
            old_cross_ref, old_tiles_ref = refs[:2]
            cross_ref[:, :first] = old_cross_ref[:, :first]
            tiles_ref[:at, :] = old_tiles_ref[:at, :]
        best(scale, part_ref, unit_ref, tiles_ref, right_at=at, left_ref=cross_ref, left_from=first)


def join_kernel(
    role_ref, own_ref, own_partner_ref, own_far_ref, far_ref, tiles_ref, rows_ref, cross_ref, ends_ref, out_ref
):
    turn, step, middle = place(role_ref)
    tiles, _ = own_ref.shape
    across = tiles // 2

    def put(slots, *values):
        slot = slots[0]
        for i in range(1, 4):
            slot = jnp.where(turn == i, slots[i], slot)
        at = pl.multiple_of(slot * tiles, tiles)
        out_ref[pl.ds(at, tiles), :] = jnp.concatenate(values[1:], axis=values[0])

    put((2, 2, 2, 2), 0, own_ref[...])
    put((4, 4, 0, 0), 0, own_partner_ref[...])
    put((3, 0, 4, 1), 0, own_far_ref[...])
    put((0, 1, 3, 4), 0, far_ref[:tiles, :])

    @pl.when(middle)
    def _():
        put((0, 3, 1, 0), 0, far_ref[tiles:, :])

    @pl.when(jnp.logical_and(jnp.logical_not(middle), step == 0))
    def _():
        put((1, 1, 1, 3), 1, rows_ref[...], cross_ref[...])

    @pl.when(jnp.logical_and(jnp.logical_not(middle), step == 1))
    def _():
        low = jnp.concatenate([ends_ref[:across, :], ends_ref[across:, :]], axis=1)
        put((1, 1, 1, 3), 0, low, tiles_ref[...])


def call(kernel, outs, *operands, last=False):
    specs, placed = [], []
    for value in operands:
        scalar = value.dtype == jnp.int32
        specs.append(pl.BlockSpec(memory_space=pltpu.SMEM if scalar else pltpu.VMEM))
        placed.append(value if scalar else pltpu.with_memory_space_constraint(value, pltpu.VMEM))
    return pl.pallas_call(
        kernel,
        out_shape=[jax.ShapeDtypeStruct(*o) if last else pltpu.VMEM(*o) for o in outs],
        in_specs=specs,
        out_specs=[pl.BlockSpec(memory_space=pltpu.VMEM) for _ in outs],
        compiler_params=pltpu.CompilerParams(vmem_limit_bytes=VMEM_LIMIT),
    )(*placed)


def body(embeddings):
    count, width = embeddings.shape
    blocks = lax.axis_size(AXES[0]) * lax.axis_size(AXES[1])
    columns = blocks // 4
    scale = 1.0 / width**0.5
    tiles, half = count // TILE, count // 2
    across, size = half // TILE, half // PARTS
    assert blocks % 8 == 0 and size % STEP == 0

    at = lambda column, turn: column % columns * 4 + turn
    far, swap, even, odd, rows, cross, ends = [], [], [], [], [], [], []
    for q in range(columns):
        far += [(at(q, 1), at(q, 0)), (at(q, 2), at(q, 3))]
        far += [(at(q, 3), at(q + 1, 1)), (at(q, 0), at(q - 1, 2))]
        swap += [(at(q, 0), at(q, 2)), (at(q, 2), at(q, 0)), (at(q, 1), at(q, 3)), (at(q, 3), at(q, 1))]
        if q % 2 == 0:
            even += [(at(q, 1), at(q, 2)), (at(q, 2), at(q, 1))]
            odd += [(at(q, 3), at(q + 1, 0)), (at(q, 0), at(q - 1, 3))]
            rows += [(at(q, 1), at(q, 0)), (at(q, 2), at(q, 3))]
            ends += [(at(q, 1), at(q - 1, 3)), (at(q, 2), at(q + 1, 0))]
        else:
            for ring in (
                (at(q, 0), at(q - 1, 3), at(q - 1, 1), at(q, 2)),
                (at(q, 3), at(q + 1, 0), at(q + 1, 2), at(q, 1)),
            ):
                cross += [(ring[i], ring[(i + 1) % 4]) for i in range(4)]

    def send(value, pairs):
        return lax.ppermute(value, AXES, pairs)

    role = lax.axis_index(AXES).astype(jnp.int32).reshape(1)
    role, embeddings = lax.optimization_barrier((role, embeddings))
    far_rows = send(embeddings, far)
    partner_rows = send(embeddings, swap)
    piece = ((size, width), BF16)
    unit, own, *odd_parts = call(
        functools.partial(own_kernel, scale),
        [((count, width), BF16), ((tiles, count), F32)] + [piece] * PARTS,
        embeddings,
    )
    odd_parts = [send(part, odd) for part in odd_parts]
    partner, *even_parts = call(partner_kernel, [((count, width), BF16)] + [piece] * PARTS, partner_rows)
    even_parts = [send(part, even) for part in even_parts]
    (own_partner,) = call(functools.partial(pair_kernel, scale), [((tiles, count), F32)], unit, partner)
    far_unit, own_far, far_max = call(
        functools.partial(far_kernel, scale),
        [((count, width), BF16), ((tiles, count), F32), ((2 * tiles, count), F32)],
        role,
        far_rows,
        unit,
        partner,
    )
    far_max = send(far_max, [(b, a) for a, b in far])
    column = ((tiles, half), F32)
    done = []
    for i, part in enumerate(even_parts):
        done = call(functools.partial(even_kernel, i * size, scale), [column, column], role, part, far_unit, *done)
    rows_max, ends_max = done
    ends_max = send(ends_max, ends)
    rows_max = send(rows_max, rows)
    done = []
    for i, part in enumerate(odd_parts):
        done = call(
            functools.partial(odd_kernel, i * size, scale), [column, ((across, count), F32)], role, part, unit, *done
        )
    cross_max, half_tiles = done
    cross_max = send(cross_max, cross)
    (out,) = call(
        join_kernel,
        [((OFFSETS * tiles, count), F32)],
        role,
        own,
        own_partner,
        own_far,
        far_max,
        half_tiles,
        rows_max,
        cross_max,
        ends_max,
        last=True,
    )
    return jnp.transpose(out)


def solution(mesh):
    return jax.shard_map(
        body,
        mesh=mesh,
        in_specs=(P(AXES, None),),
        out_specs=P(AXES, None),
        check_vma=False,
    )
```

```python
import functools

import jax
import jax.numpy as jnp
from jax import lax
from jax.experimental import pallas as pl
from jax.experimental.pallas import tpu as pltpu
from jax.sharding import PartitionSpec as P


AXES = ("blk", "grp")
TILE = 128
STEP = 256
PARTS = 2
OFFSETS = 5
VMEM_LIMIT = 16 << 20
F32, BF16 = jnp.float32, jnp.bfloat16


def unit_of(rows):
    values = rows.astype(F32)
    mean = jnp.mean(values * values, axis=-1, keepdims=True)
    return (values * lax.rsqrt(mean + 1e-06)).astype(BF16)


def scores(left, right):
    return lax.dot_general(left, right, (((1,), (1,)), ((), ())), preferred_element_type=F32)


def best(scale, left, right, right_ref, right_at=0, left_ref=None, left_at=0, left_from=0, same=None):
    rows, keys = left.shape[0], right.shape[0]
    for m in range(0, rows, STEP):
        for n in range(0, keys, STEP):
            s = scores(left[m : m + STEP, :], right[n : n + STEP, :])
            if same is not None and m == n:
                s = jnp.where(same, -jnp.inf, s)
            tiles = jnp.max(s.reshape(STEP // TILE, TILE, STEP), axis=1)
            at = right_at + m // TILE
            right_ref[at : at + STEP // TILE, n : n + STEP] = tiles * scale
            if left_ref is not None:
                for t in range(STEP // TILE):
                    tile = jnp.max(s[:, t * TILE : (t + 1) * TILE], axis=1)
                    at = left_at + n // TILE + t
                    left_ref[at : at + 1, left_from + m : left_from + m + STEP] = tile.reshape(1, STEP) * scale


def place(role_ref):
    turn = lax.rem(role_ref[0], 4)
    step = 1 - lax.rem(lax.div(role_ref[0], 4), 2)
    return turn, step, jnp.logical_or(turn == 1, turn == 2)


def own_kernel(scale, rows_ref, unit_ref, own_ref, *part_refs):
    unit_ref[...] = unit_of(rows_ref[...])
    size = part_refs[0].shape[0]
    for i, part_ref in enumerate(part_refs):
        at = (len(part_refs) + i) * size
        part_ref[...] = unit_ref[at : at + size, :]
    same = lax.broadcasted_iota(jnp.int32, (STEP, STEP), 0) == lax.broadcasted_iota(
        jnp.int32, (STEP, STEP), 1
    )
    best(scale, unit_ref, unit_ref, own_ref, same=same)


def partner_kernel(rows_ref, partner_ref, *part_refs):
    partner_ref[...] = unit_of(rows_ref[...])
    size = part_refs[0].shape[0]
    for i, part_ref in enumerate(part_refs):
        part_ref[...] = partner_ref[i * size : (i + 1) * size, :]


def pair_kernel(scale, unit_ref, partner_ref, max_ref):
    best(scale, partner_ref, unit_ref, max_ref)


def far_kernel(scale, role_ref, rows_ref, unit_ref, partner_ref, far_ref, own_far_ref, far_max_ref):
    middle = place(role_ref)[2]
    tiles = own_far_ref.shape[0]
    far_ref[...] = unit_of(rows_ref[...])
    best(scale, far_ref, unit_ref, own_far_ref, left_ref=far_max_ref)

    @pl.when(jnp.logical_not(middle))
    def _():
        best(scale, partner_ref, far_ref, far_max_ref, right_at=tiles)


def even_kernel(first, scale, role_ref, part_ref, far_ref, *refs):
    _, step, middle = place(role_ref)
    rows_ref, ends_ref = refs[-2:]
    half = far_ref.shape[0] // 2
    at, across = first // TILE, half // TILE

    @pl.when(jnp.logical_and(step == 0, middle))
    def _():
        if first:
            old_rows_ref, old_ends_ref = refs[:2]
            rows_ref[:, :first] = old_rows_ref[:, :first]
            ends_ref[:at, :] = old_ends_ref[:at, :]
            ends_ref[across : across + at, :] = old_ends_ref[across : across + at, :]
        best(scale, part_ref, far_ref.at[:half, :], ends_ref, right_at=at, left_ref=rows_ref, left_from=first)
        best(
            scale, part_ref, far_ref.at[half:, :], ends_ref, right_at=across + at,
            left_ref=rows_ref, left_at=across, left_from=first,
        )


def odd_kernel(first, scale, role_ref, part_ref, unit_ref, *refs):
    _, step, middle = place(role_ref)
    cross_ref, tiles_ref = refs[-2:]
    at = first // TILE

    @pl.when(jnp.logical_and(step == 1, jnp.logical_not(middle)))
    def _():
        if first:
            old_cross_ref, old_tiles_ref = refs[:2]
            cross_ref[:, :first] = old_cross_ref[:, :first]
            tiles_ref[:at, :] = old_tiles_ref[:at, :]
        best(scale, part_ref, unit_ref, tiles_ref, right_at=at, left_ref=cross_ref, left_from=first)


def join_kernel(
    role_ref, own_ref, own_partner_ref, own_far_ref, far_ref, tiles_ref, rows_ref, cross_ref, ends_ref, out_ref
):
    turn, step, middle = place(role_ref)
    tiles, _ = own_ref.shape
    across = tiles // 2

    def put(slots, *values):
        slot = slots[0]
        for i in range(1, 4):
            slot = jnp.where(turn == i, slots[i], slot)
        at = pl.multiple_of(slot * tiles, tiles)
        out_ref[pl.ds(at, tiles), :] = jnp.concatenate(values[1:], axis=values[0])

    put((2, 2, 2, 2), 0, own_ref[...])
    put((4, 4, 0, 0), 0, own_partner_ref[...])
    put((3, 0, 4, 1), 0, own_far_ref[...])
    put((0, 1, 3, 4), 0, far_ref[:tiles, :])

    @pl.when(middle)
    def _():
        put((0, 3, 1, 0), 0, far_ref[tiles:, :])

    @pl.when(jnp.logical_and(jnp.logical_not(middle), step == 0))
    def _():
        put((1, 1, 1, 3), 1, rows_ref[...], cross_ref[...])

    @pl.when(jnp.logical_and(jnp.logical_not(middle), step == 1))
    def _():
        low = jnp.concatenate([ends_ref[:across, :], ends_ref[across:, :]], axis=1)
        put((1, 1, 1, 3), 0, low, tiles_ref[...])


def call(kernel, outs, *operands, last=False):
    specs, placed = [], []
    for value in operands:
        scalar = value.dtype == jnp.int32
        specs.append(pl.BlockSpec(memory_space=pltpu.SMEM if scalar else pltpu.VMEM))
        placed.append(value if scalar else pltpu.with_memory_space_constraint(value, pltpu.VMEM))
    return pl.pallas_call(
        kernel,
        out_shape=[jax.ShapeDtypeStruct(*o) if last else pltpu.VMEM(*o) for o in outs],
        in_specs=specs,
        out_specs=[pl.BlockSpec(memory_space=pltpu.VMEM) for _ in outs],
        compiler_params=pltpu.CompilerParams(vmem_limit_bytes=VMEM_LIMIT),
    )(*placed)


def ring_pairs(ring):
    return list(zip(ring, ring[1:] + ring[:1]))


def body(embeddings):
    count, width = embeddings.shape
    blocks = lax.axis_size(AXES[0]) * lax.axis_size(AXES[1])
    columns = blocks // 4
    scale = 1.0 / width**0.5
    tiles, half = count // TILE, count // 2
    across, size = half // TILE, half // PARTS
    assert blocks % 8 == 0 and size % STEP == 0

    at = lambda column, turn: column % columns * 4 + turn
    far, swap, even, odd, rows, cross, ends = [], [], [], [], [], [], []
    for q in range(columns):
        far += [(at(q, 1), at(q, 0)), (at(q, 2), at(q, 3))]
        far += [(at(q, 3), at(q + 1, 1)), (at(q, 0), at(q - 1, 2))]
        swap += [(at(q, 0), at(q, 2)), (at(q, 2), at(q, 0)), (at(q, 1), at(q, 3)), (at(q, 3), at(q, 1))]
        if q % 2 == 1:
            even += [(at(q, 1), at(q, 2)), (at(q, 2), at(q, 1))]
            odd += [(at(q, 3), at(q + 1, 0)), (at(q, 0), at(q - 1, 3))]
            rows += [(at(q, 1), at(q, 0)), (at(q, 2), at(q, 3))]
            for ring in (
                (at(q, 1), at(q - 1, 3), at(q - 1, 1)),
                (at(q, 2), at(q + 1, 0), at(q + 1, 2)),
                (at(q, 0), at(q, 3)),
            ):
                ends += ring_pairs(ring)
        else:
            for ring in (
                (at(q, 0), at(q - 1, 3), at(q - 1, 1), at(q, 2)),
                (at(q, 3), at(q + 1, 0), at(q + 1, 2), at(q, 1)),
            ):
                cross += ring_pairs(ring)

    def send(value, pairs):
        return lax.ppermute(value, AXES, pairs)

    role = lax.axis_index(AXES).astype(jnp.int32).reshape(1)
    role, embeddings = lax.optimization_barrier((role, embeddings))
    far_rows = send(embeddings, far)
    partner_rows = send(embeddings, swap)
    piece = ((size, width), BF16)
    unit, own, *odd_parts = call(
        functools.partial(own_kernel, scale),
        [((count, width), BF16), ((tiles, count), F32)] + [piece] * PARTS,
        embeddings,
    )
    odd_parts = [send(part, odd) for part in odd_parts]
    partner, *even_parts = call(partner_kernel, [((count, width), BF16)] + [piece] * PARTS, partner_rows)
    even_parts = [send(part, even) for part in even_parts]
    (own_partner,) = call(functools.partial(pair_kernel, scale), [((tiles, count), F32)], unit, partner)
    far_unit, own_far, far_max = call(
        functools.partial(far_kernel, scale),
        [((count, width), BF16), ((tiles, count), F32), ((2 * tiles, count), F32)],
        role,
        far_rows,
        unit,
        partner,
    )
    far_max = send(far_max, [(b, a) for a, b in far])
    column = ((tiles, half), F32)
    done = []
    for i, part in enumerate(even_parts):
        done = call(functools.partial(even_kernel, i * size, scale), [column, column], role, part, far_unit, *done)
    rows_max, ends_max = done
    ends_max = send(ends_max, ends)
    rows_max = send(rows_max, rows)
    done = []
    for i, part in enumerate(odd_parts):
        done = call(
            functools.partial(odd_kernel, i * size, scale), [column, ((across, count), F32)], role, part, unit, *done
        )
    cross_max, half_tiles = done
    cross_max = send(cross_max, cross)
    (out,) = call(
        join_kernel,
        [((OFFSETS * tiles, count), F32)],
        role,
        own,
        own_partner,
        own_far,
        far_max,
        half_tiles,
        rows_max,
        cross_max,
        ends_max,
        last=True,
    )
    return jnp.transpose(out)


def solution(mesh):
    return jax.shard_map(
        body,
        mesh=mesh,
        in_specs=(P(AXES, None),),
        out_specs=P(AXES, None),
        check_vma=False,
    )
```

```python
import functools

import jax
import jax.numpy as jnp
from jax import lax
from jax.experimental import pallas as pl
from jax.experimental.pallas import tpu as pltpu
from jax.sharding import PartitionSpec as P


AXES = ("blk", "grp")
TILE = 128
STEP = 256
PARTS = 1
OFFSETS = 5
VMEM_LIMIT = 16 << 20
F32, BF16 = jnp.float32, jnp.bfloat16


def unit_of(rows):
    values = rows.astype(F32)
    mean = jnp.mean(values * values, axis=-1, keepdims=True)
    return (values * lax.rsqrt(mean + 1e-06)).astype(BF16)


def scores(left, right):
    return lax.dot_general(left, right, (((1,), (1,)), ((), ())), preferred_element_type=F32)


def best(scale, left, right, right_ref, right_at=0, left_ref=None, left_at=0, left_from=0, same=None):
    rows, keys = left.shape[0], right.shape[0]
    for m in range(0, rows, STEP):
        for n in range(0, keys, STEP):
            s = scores(left[m : m + STEP, :], right[n : n + STEP, :])
            if same is not None and m == n:
                s = jnp.where(same, -jnp.inf, s)
            tiles = jnp.max(s.reshape(STEP // TILE, TILE, STEP), axis=1)
            at = right_at + m // TILE
            right_ref[at : at + STEP // TILE, n : n + STEP] = tiles * scale
            if left_ref is not None:
                for t in range(STEP // TILE):
                    tile = jnp.max(s[:, t * TILE : (t + 1) * TILE], axis=1)
                    at = left_at + n // TILE + t
                    left_ref[at : at + 1, left_from + m : left_from + m + STEP] = tile.reshape(1, STEP) * scale


def place(role_ref):
    turn = lax.rem(role_ref[0], 4)
    step = 1 - lax.rem(lax.div(role_ref[0], 4), 2)
    return turn, step, jnp.logical_or(turn == 1, turn == 2)


def own_kernel(scale, rows_ref, unit_ref, own_ref, *part_refs):
    unit_ref[...] = unit_of(rows_ref[...])
    size = part_refs[0].shape[0]
    for i, part_ref in enumerate(part_refs):
        at = (len(part_refs) + i) * size
        part_ref[...] = unit_ref[at : at + size, :]
    same = lax.broadcasted_iota(jnp.int32, (STEP, STEP), 0) == lax.broadcasted_iota(
        jnp.int32, (STEP, STEP), 1
    )
    best(scale, unit_ref, unit_ref, own_ref, same=same)


def partner_kernel(rows_ref, partner_ref, *part_refs):
    partner_ref[...] = unit_of(rows_ref[...])
    size = part_refs[0].shape[0]
    for i, part_ref in enumerate(part_refs):
        part_ref[...] = partner_ref[i * size : (i + 1) * size, :]


def pair_kernel(scale, unit_ref, partner_ref, max_ref):
    best(scale, partner_ref, unit_ref, max_ref)


def far_kernel(scale, role_ref, rows_ref, unit_ref, partner_ref, far_ref, own_far_ref, far_max_ref):
    middle = place(role_ref)[2]
    tiles = own_far_ref.shape[0]
    far_ref[...] = unit_of(rows_ref[...])
    best(scale, far_ref, unit_ref, own_far_ref, left_ref=far_max_ref)

    @pl.when(jnp.logical_not(middle))
    def _():
        best(scale, partner_ref, far_ref, far_max_ref, right_at=tiles)


def even_kernel(first, scale, role_ref, part_ref, far_ref, *refs):
    _, step, middle = place(role_ref)
    rows_ref, ends_ref = refs[-2:]
    half = far_ref.shape[0] // 2
    at, across = first // TILE, half // TILE

    @pl.when(jnp.logical_and(step == 0, middle))
    def _():
        if first:
            old_rows_ref, old_ends_ref = refs[:2]
            rows_ref[:, :first] = old_rows_ref[:, :first]
            ends_ref[:at, :] = old_ends_ref[:at, :]
            ends_ref[across : across + at, :] = old_ends_ref[across : across + at, :]
        best(scale, part_ref, far_ref.at[:half, :], ends_ref, right_at=at, left_ref=rows_ref, left_from=first)
        best(
            scale, part_ref, far_ref.at[half:, :], ends_ref, right_at=across + at,
            left_ref=rows_ref, left_at=across, left_from=first,
        )


def odd_kernel(first, scale, role_ref, part_ref, unit_ref, *refs):
    _, step, middle = place(role_ref)
    cross_ref, tiles_ref = refs[-2:]
    at = first // TILE

    @pl.when(jnp.logical_and(step == 1, jnp.logical_not(middle)))
    def _():
        if first:
            old_cross_ref, old_tiles_ref = refs[:2]
            cross_ref[:, :first] = old_cross_ref[:, :first]
            tiles_ref[:at, :] = old_tiles_ref[:at, :]
        best(scale, part_ref, unit_ref, tiles_ref, right_at=at, left_ref=cross_ref, left_from=first)


def join_kernel(
    role_ref, own_ref, own_partner_ref, own_far_ref, far_ref, tiles_ref, rows_ref, cross_ref, ends_ref, out_ref
):
    turn, step, middle = place(role_ref)
    tiles, _ = own_ref.shape
    across = tiles // 2

    def put(slots, *values):
        slot = slots[0]
        for i in range(1, 4):
            slot = jnp.where(turn == i, slots[i], slot)
        at = pl.multiple_of(slot * tiles, tiles)
        out_ref[pl.ds(at, tiles), :] = jnp.concatenate(values[1:], axis=values[0])

    put((2, 2, 2, 2), 0, own_ref[...])
    put((4, 4, 0, 0), 0, own_partner_ref[...])
    put((3, 0, 4, 1), 0, own_far_ref[...])
    put((0, 1, 3, 4), 0, far_ref[:tiles, :])

    @pl.when(middle)
    def _():
        put((0, 3, 1, 0), 0, far_ref[tiles:, :])

    @pl.when(jnp.logical_and(jnp.logical_not(middle), step == 0))
    def _():
        put((1, 1, 1, 3), 1, rows_ref[...], cross_ref[...])

    @pl.when(jnp.logical_and(jnp.logical_not(middle), step == 1))
    def _():
        low = jnp.concatenate([ends_ref[:across, :], ends_ref[across:, :]], axis=1)
        put((1, 1, 1, 3), 0, low, tiles_ref[...])


def call(kernel, outs, *operands, last=False):
    specs, placed = [], []
    for value in operands:
        scalar = value.dtype == jnp.int32
        specs.append(pl.BlockSpec(memory_space=pltpu.SMEM if scalar else pltpu.VMEM))
        placed.append(value if scalar else pltpu.with_memory_space_constraint(value, pltpu.VMEM))
    return pl.pallas_call(
        kernel,
        out_shape=[jax.ShapeDtypeStruct(*o) if last else pltpu.VMEM(*o) for o in outs],
        in_specs=specs,
        out_specs=[pl.BlockSpec(memory_space=pltpu.VMEM) for _ in outs],
        compiler_params=pltpu.CompilerParams(vmem_limit_bytes=VMEM_LIMIT),
    )(*placed)


def body(embeddings):
    count, width = embeddings.shape
    blocks = lax.axis_size(AXES[0]) * lax.axis_size(AXES[1])
    columns = blocks // 4
    scale = 1.0 / width**0.5
    tiles, half = count // TILE, count // 2
    across, size = half // TILE, half // PARTS
    assert blocks % 8 == 0 and size % STEP == 0

    at = lambda column, turn: column % columns * 4 + turn
    far, swap, even, odd, rows, cross, ends = [], [], [], [], [], [], []
    for q in range(columns):
        far += [(at(q, 1), at(q, 0)), (at(q, 2), at(q, 3))]
        far += [(at(q, 3), at(q + 1, 1)), (at(q, 0), at(q - 1, 2))]
        swap += [(at(q, 0), at(q, 2)), (at(q, 2), at(q, 0)), (at(q, 1), at(q, 3)), (at(q, 3), at(q, 1))]
        beside = q ^ 1
        if q % 2 == 1:
            even += [(at(q, 1), at(q, 2)), (at(q, 2), at(q, 1))]
            odd += [(at(q, 3), at(q + 1, 0)), (at(q, 0), at(q - 1, 3))]
            rows += [(at(q, 1), at(q, 0)), (at(q, 2), at(q, 3))]
            ends += [(at(q, 1), at(q - 1, 3)), (at(q, 2), at(q + 1, 0))]
            ends += [(at(q, 0), at(q, 3)), (at(q, 3), at(q, 0))]
            cross += [(at(q, 3), at(q, 1)), (at(q, 0), at(q, 2))]
            cross += [(at(q, 1), at(beside, 1)), (at(q, 2), at(beside, 2))]
        else:
            cross += [(at(q, 0), at(q - 1, 3)), (at(q, 3), at(q + 1, 0))]
            cross += [(at(q, 1), at(q, 3)), (at(q, 2), at(q, 0))]
            ends += [(at(q, 3), at(q, 1)), (at(q, 0), at(q, 2))]
            ends += [(at(q, 1), at(beside, 1)), (at(q, 2), at(beside, 2))]

    def send(value, pairs):
        return lax.ppermute(value, AXES, pairs)

    role = lax.axis_index(AXES).astype(jnp.int32).reshape(1)
    role, embeddings = lax.optimization_barrier((role, embeddings))
    far_rows = send(embeddings, far)
    partner_rows = send(embeddings, swap)
    piece = ((size, width), BF16)
    unit, own, *odd_parts = call(
        functools.partial(own_kernel, scale),
        [((count, width), BF16), ((tiles, count), F32)] + [piece] * PARTS,
        embeddings,
    )
    odd_parts = [send(part, odd) for part in odd_parts]
    partner, *even_parts = call(partner_kernel, [((count, width), BF16)] + [piece] * PARTS, partner_rows)
    even_parts = [send(part, even) for part in even_parts]
    (own_partner,) = call(functools.partial(pair_kernel, scale), [((tiles, count), F32)], unit, partner)
    far_unit, own_far, far_max = call(
        functools.partial(far_kernel, scale),
        [((count, width), BF16), ((tiles, count), F32), ((2 * tiles, count), F32)],
        role,
        far_rows,
        unit,
        partner,
    )
    far_max = send(far_max, [(b, a) for a, b in far])
    column = ((tiles, half), F32)
    done = []
    for i, part in enumerate(even_parts):
        done = call(functools.partial(even_kernel, i * size, scale), [column, column], role, part, far_unit, *done)
    rows_max, ends_max = done
    ends_max = send(ends_max, ends)
    rows_max = send(rows_max, rows)
    done = []
    for i, part in enumerate(odd_parts):
        done = call(
            functools.partial(odd_kernel, i * size, scale), [column, ((across, count), F32)], role, part, unit, *done
        )
    cross_max, half_tiles = done
    cross_max = send(cross_max, cross)
    (out,) = call(
        join_kernel,
        [((OFFSETS * tiles, count), F32)],
        role,
        own,
        own_partner,
        own_far,
        far_max,
        half_tiles,
        rows_max,
        cross_max,
        ends_max,
        last=True,
    )
    return jnp.transpose(out)


def solution(mesh):
    return jax.shard_map(
        body,
        mesh=mesh,
        in_specs=(P(AXES, None),),
        out_specs=P(AXES, None),
        check_vma=False,
    )
```

```python
import functools

import jax
import jax.numpy as jnp
from jax import lax
from jax.experimental import pallas as pl
from jax.experimental.pallas import tpu as pltpu
from jax.sharding import PartitionSpec as P


AXES = ("blk", "grp")
TILE = 128
STEP = 256
PARTS = 2
OFFSETS = 5
VMEM_LIMIT = 16 << 20
F32, BF16 = jnp.float32, jnp.bfloat16


def unit_of(rows):
    values = rows.astype(F32)
    mean = jnp.mean(values * values, axis=-1, keepdims=True)
    return (values * lax.rsqrt(mean + 1e-06)).astype(BF16)


def scores(left, right):
    return lax.dot_general(left, right, (((1,), (1,)), ((), ())), preferred_element_type=F32)


def best(scale, left, right, right_ref, right_at=0, left_ref=None, left_at=0, left_from=0, same=None):
    rows, keys = left.shape[0], right.shape[0]
    for m in range(0, rows, STEP):
        for n in range(0, keys, STEP):
            s = scores(left[m : m + STEP, :], right[n : n + STEP, :])
            if same is not None and m == n:
                s = jnp.where(same, -jnp.inf, s)
            tiles = jnp.max(s.reshape(STEP // TILE, TILE, STEP), axis=1)
            at = right_at + m // TILE
            right_ref[at : at + STEP // TILE, n : n + STEP] = tiles * scale
            if left_ref is not None:
                for t in range(STEP // TILE):
                    tile = jnp.max(s[:, t * TILE : (t + 1) * TILE], axis=1)
                    at = left_at + n // TILE + t
                    left_ref[at : at + 1, left_from + m : left_from + m + STEP] = tile.reshape(1, STEP) * scale


def place(role_ref):
    turn = lax.rem(role_ref[0], 4)
    step = 1 - lax.rem(lax.div(role_ref[0], 4), 2)
    return turn, step, jnp.logical_or(turn == 1, turn == 2)


def own_kernel(scale, rows_ref, unit_ref, own_ref, *part_refs):
    unit_ref[...] = unit_of(rows_ref[...])
    size = part_refs[0].shape[0]
    for i, part_ref in enumerate(part_refs):
        part_ref[...] = unit_ref[i * size : (i + 1) * size, :]
    same = lax.broadcasted_iota(jnp.int32, (STEP, STEP), 0) == lax.broadcasted_iota(
        jnp.int32, (STEP, STEP), 1
    )
    best(scale, unit_ref, unit_ref, own_ref, same=same)


def partner_kernel(rows_ref, partner_ref):
    partner_ref[...] = unit_of(rows_ref[...])


def pair_kernel(scale, unit_ref, partner_ref, max_ref):
    best(scale, partner_ref, unit_ref, max_ref)


def far_kernel(scale, role_ref, rows_ref, unit_ref, partner_ref, far_ref, own_far_ref, far_max_ref):
    middle = place(role_ref)[2]
    tiles = own_far_ref.shape[0]
    far_ref[...] = unit_of(rows_ref[...])
    best(scale, far_ref, unit_ref, own_far_ref, left_ref=far_max_ref)

    @pl.when(jnp.logical_not(middle))
    def _():
        best(scale, partner_ref, far_ref, far_max_ref, right_at=tiles)


def even_kernel(first, scale, role_ref, part_ref, far_ref, *refs):
    _, step, middle = place(role_ref)
    rows_ref, ends_ref = refs[-2:]
    half = far_ref.shape[0] // 2
    at, across = first // TILE, half // TILE

    @pl.when(jnp.logical_and(step == 0, middle))
    def _():
        if first:
            old_rows_ref, old_ends_ref = refs[:2]
            rows_ref[:, :first] = old_rows_ref[:, :first]
            ends_ref[:at, :] = old_ends_ref[:at, :]
            ends_ref[across : across + at, :] = old_ends_ref[across : across + at, :]
        best(scale, part_ref, far_ref.at[:half, :], ends_ref, right_at=at, left_ref=rows_ref, left_from=first)
        best(
            scale, part_ref, far_ref.at[half:, :], ends_ref, right_at=across + at,
            left_ref=rows_ref, left_at=across, left_from=first,
        )


def odd_kernel(first, scale, role_ref, part_ref, unit_ref, *refs):
    _, step, middle = place(role_ref)
    cross_ref, tiles_ref = refs[-2:]
    at = first // TILE

    @pl.when(jnp.logical_and(step == 1, jnp.logical_not(middle)))
    def _():
        if first:
            old_cross_ref, old_tiles_ref = refs[:2]
            cross_ref[:, :first] = old_cross_ref[:, :first]
            tiles_ref[:at, :] = old_tiles_ref[:at, :]
        best(scale, part_ref, unit_ref, tiles_ref, right_at=at, left_ref=cross_ref, left_from=first)


def join_kernel(
    role_ref, own_ref, own_partner_ref, own_far_ref, far_ref, tiles_ref, rows_ref, cross_ref, ends_ref, out_ref
):
    turn, step, middle = place(role_ref)
    tiles, _ = own_ref.shape
    across = tiles // 2

    def put(slots, *values):
        slot = slots[0]
        for i in range(1, 4):
            slot = jnp.where(turn == i, slots[i], slot)
        at = pl.multiple_of(slot * tiles, tiles)
        out_ref[pl.ds(at, tiles), :] = jnp.concatenate(values[1:], axis=values[0])

    put((2, 2, 2, 2), 0, own_ref[...])
    put((4, 4, 0, 0), 0, own_partner_ref[...])
    put((3, 0, 4, 1), 0, own_far_ref[...])
    put((0, 1, 3, 4), 0, far_ref[:tiles, :])

    @pl.when(middle)
    def _():
        put((0, 3, 1, 0), 0, far_ref[tiles:, :])

    @pl.when(jnp.logical_and(jnp.logical_not(middle), step == 0))
    def _():
        put((1, 1, 1, 3), 1, rows_ref[...], cross_ref[...])

    @pl.when(jnp.logical_and(jnp.logical_not(middle), step == 1))
    def _():
        low = jnp.concatenate([ends_ref[:across, :], ends_ref[across:, :]], axis=1)
        put((1, 1, 1, 3), 0, low, tiles_ref[...])


def call(kernel, outs, *operands, last=False):
    specs, placed = [], []
    for value in operands:
        scalar = value.dtype == jnp.int32
        specs.append(pl.BlockSpec(memory_space=pltpu.SMEM if scalar else pltpu.VMEM))
        placed.append(value if scalar else pltpu.with_memory_space_constraint(value, pltpu.VMEM))
    return pl.pallas_call(
        kernel,
        out_shape=[jax.ShapeDtypeStruct(*o) if last else pltpu.VMEM(*o) for o in outs],
        in_specs=specs,
        out_specs=[pl.BlockSpec(memory_space=pltpu.VMEM) for _ in outs],
        compiler_params=pltpu.CompilerParams(vmem_limit_bytes=VMEM_LIMIT),
    )(*placed)


def body(embeddings):
    count, width = embeddings.shape
    blocks = lax.axis_size(AXES[0]) * lax.axis_size(AXES[1])
    columns = blocks // 4
    scale = 1.0 / width**0.5
    tiles, half = count // TILE, count // 2
    across, size = half // TILE, half // PARTS
    assert blocks % 8 == 0 and size % STEP == 0

    at = lambda column, turn: column % columns * 4 + turn
    far, swap, even, odd, rows, cross, ends = [], [], [], [], [], [], []
    for q in range(columns):
        far += [(at(q, 1), at(q, 0)), (at(q, 2), at(q, 3))]
        far += [(at(q, 3), at(q + 1, 1)), (at(q, 0), at(q - 1, 2))]
        swap += [(at(q, 0), at(q, 2)), (at(q, 2), at(q, 0)), (at(q, 1), at(q, 3)), (at(q, 3), at(q, 1))]
        beside = q ^ 1
        if q % 2 == 1:
            even += [(at(q, 3), at(q, 2)), (at(q, 0), at(q, 1))]
            odd += [(at(q, 3), at(q + 1, 0)), (at(q, 0), at(q - 1, 3))]
            rows += [(at(q, 1), at(q, 0)), (at(q, 2), at(q, 3))]
            ends += [(at(q, 1), at(q - 1, 3)), (at(q, 2), at(q + 1, 0))]
            ends += [(at(q, 0), at(q, 3)), (at(q, 3), at(q, 0))]
            cross += [(at(q, 3), at(q, 1)), (at(q, 0), at(q, 2))]
            cross += [(at(q, 1), at(beside, 1)), (at(q, 2), at(beside, 2))]
        else:
            cross += [(at(q, 0), at(q - 1, 3)), (at(q, 3), at(q + 1, 0))]
            cross += [(at(q, 1), at(q, 3)), (at(q, 2), at(q, 0))]
            ends += [(at(q, 3), at(q, 1)), (at(q, 0), at(q, 2))]
            ends += [(at(q, 1), at(beside, 1)), (at(q, 2), at(beside, 2))]

    def send(value, pairs):
        return lax.ppermute(value, AXES, pairs)

    role = lax.axis_index(AXES).astype(jnp.int32).reshape(1)
    role, embeddings = lax.optimization_barrier((role, embeddings))
    far_rows = send(embeddings, far)
    partner_rows = send(embeddings, swap)
    piece = ((size, width), BF16)
    unit, own, *pieces = call(
        functools.partial(own_kernel, scale),
        [((count, width), BF16), ((tiles, count), F32)] + [piece] * (2 * PARTS),
        embeddings,
    )
    (partner,) = call(partner_kernel, [((count, width), BF16)], partner_rows)
    (own_partner,) = call(functools.partial(pair_kernel, scale), [((tiles, count), F32)], unit, partner)
    pieces, own_partner = lax.optimization_barrier((pieces, own_partner))
    odd_parts = [send(part, odd) for part in pieces[PARTS:]]
    even_parts = [send(part, even) for part in pieces[:PARTS]]
    far_unit, own_far, far_max = call(
        functools.partial(far_kernel, scale),
        [((count, width), BF16), ((tiles, count), F32), ((2 * tiles, count), F32)],
        role,
        far_rows,
        unit,
        partner,
    )
    far_max = send(far_max, [(b, a) for a, b in far])
    column = ((tiles, half), F32)
    done = []
    for i, part in enumerate(even_parts):
        done = call(functools.partial(even_kernel, i * size, scale), [column, column], role, part, far_unit, *done)
    rows_max, ends_max = done
    ends_max = send(ends_max, ends)
    rows_max = send(rows_max, rows)
    done = []
    for i, part in enumerate(odd_parts):
        done = call(
            functools.partial(odd_kernel, i * size, scale), [column, ((across, count), F32)], role, part, unit, *done
        )
    cross_max, half_tiles = done
    cross_max = send(cross_max, cross)
    (out,) = call(
        join_kernel,
        [((OFFSETS * tiles, count), F32)],
        role,
        own,
        own_partner,
        own_far,
        far_max,
        half_tiles,
        rows_max,
        cross_max,
        ends_max,
        last=True,
    )
    return jnp.transpose(out)


def solution(mesh):
    return jax.shard_map(
        body,
        mesh=mesh,
        in_specs=(P(AXES, None),),
        out_specs=P(AXES, None),
        check_vma=False,
    )
```

```python
import functools

import jax
import jax.numpy as jnp
from jax import lax
from jax.experimental import pallas as pl
from jax.experimental.pallas import tpu as pltpu
from jax.sharding import PartitionSpec as P


AXES = ("blk", "grp")
TILE = 128
STEP = 256
PARTS = 2
OFFSETS = 5
VMEM_LIMIT = 16 << 20
F32, BF16 = jnp.float32, jnp.bfloat16


def unit_of(rows):
    values = rows.astype(F32)
    mean = jnp.mean(values * values, axis=-1, keepdims=True)
    return (values * lax.rsqrt(mean + 1e-06)).astype(BF16)


def scores(left, right):
    return lax.dot_general(left, right, (((1,), (1,)), ((), ())), preferred_element_type=F32)


def best(scale, left, right, right_ref, right_at=0, left_ref=None, left_at=0, left_from=0, same=None):
    rows, keys = left.shape[0], right.shape[0]
    for m in range(0, rows, STEP):
        for n in range(0, keys, STEP):
            s = scores(left[m : m + STEP, :], right[n : n + STEP, :])
            if same is not None and m == n:
                s = jnp.where(same, -jnp.inf, s)
            tiles = jnp.max(s.reshape(STEP // TILE, TILE, STEP), axis=1)
            at = right_at + m // TILE
            right_ref[at : at + STEP // TILE, n : n + STEP] = tiles * scale
            if left_ref is not None:
                for t in range(STEP // TILE):
                    tile = jnp.max(s[:, t * TILE : (t + 1) * TILE], axis=1)
                    at = left_at + n // TILE + t
                    left_ref[at : at + 1, left_from + m : left_from + m + STEP] = tile.reshape(1, STEP) * scale


def place(role_ref):
    turn = lax.rem(role_ref[0], 4)
    step = 1 - lax.rem(lax.div(role_ref[0], 4), 2)
    return turn, step, jnp.logical_or(turn == 1, turn == 2)


def own_kernel(scale, rows_ref, unit_ref, own_ref, *part_refs):
    unit_ref[...] = unit_of(rows_ref[...])
    size = part_refs[0].shape[0]
    for i, part_ref in enumerate(part_refs):
        at = (len(part_refs) + i) * size
        part_ref[...] = unit_ref[at : at + size, :]
    same = lax.broadcasted_iota(jnp.int32, (STEP, STEP), 0) == lax.broadcasted_iota(
        jnp.int32, (STEP, STEP), 1
    )
    best(scale, unit_ref, unit_ref, own_ref, same=same)


def partner_kernel(rows_ref, partner_ref, *part_refs):
    partner_ref[...] = unit_of(rows_ref[...])
    size = part_refs[0].shape[0]
    for i, part_ref in enumerate(part_refs):
        part_ref[...] = partner_ref[i * size : (i + 1) * size, :]


def pair_kernel(scale, unit_ref, partner_ref, max_ref):
    best(scale, partner_ref, unit_ref, max_ref)


def far_kernel(scale, role_ref, rows_ref, unit_ref, partner_ref, far_ref, own_far_ref, far_max_ref, beside_ref):
    middle = place(role_ref)[2]
    far_ref[...] = unit_of(rows_ref[...])
    best(scale, far_ref, unit_ref, own_far_ref, left_ref=far_max_ref)

    @pl.when(jnp.logical_not(middle))
    def _():
        best(scale, far_ref, partner_ref, beside_ref)


def even_kernel(first, scale, role_ref, part_ref, far_ref, *refs):
    _, step, middle = place(role_ref)
    rows_ref, ends_ref = refs[-2:]
    half = far_ref.shape[0] // 2
    at, across = first // TILE, half // TILE

    @pl.when(jnp.logical_and(step == 0, middle))
    def _():
        if first:
            old_rows_ref, old_ends_ref = refs[:2]
            rows_ref[:, :first] = old_rows_ref[:, :first]
            ends_ref[:at, :] = old_ends_ref[:at, :]
            ends_ref[across : across + at, :] = old_ends_ref[across : across + at, :]
        best(scale, part_ref, far_ref.at[:half, :], ends_ref, right_at=at, left_ref=rows_ref, left_from=first)
        best(
            scale, part_ref, far_ref.at[half:, :], ends_ref, right_at=across + at,
            left_ref=rows_ref, left_at=across, left_from=first,
        )


def odd_kernel(first, scale, role_ref, part_ref, unit_ref, *refs):
    _, step, middle = place(role_ref)
    cross_ref, tiles_ref = refs[-2:]
    at = first // TILE

    @pl.when(jnp.logical_and(step == 1, jnp.logical_not(middle)))
    def _():
        if first:
            old_cross_ref, old_tiles_ref = refs[:2]
            cross_ref[:, :first] = old_cross_ref[:, :first]
            tiles_ref[:at, :] = old_tiles_ref[:at, :]
        best(scale, part_ref, unit_ref, tiles_ref, right_at=at, left_ref=cross_ref, left_from=first)


def join_kernel(
    role_ref, own_ref, own_partner_ref, own_far_ref, far_ref, beside_ref, tiles_ref, rows_ref, cross_ref,
    ends_ref, out_ref
):
    turn, step, middle = place(role_ref)
    tiles, _ = own_ref.shape
    across = tiles // 2

    def put(slots, *values):
        slot = slots[0]
        for i in range(1, 4):
            slot = jnp.where(turn == i, slots[i], slot)
        at = pl.multiple_of(slot * tiles, tiles)
        out_ref[pl.ds(at, tiles), :] = jnp.concatenate(values[1:], axis=values[0])

    put((2, 2, 2, 2), 0, own_ref[...])
    put((4, 4, 0, 0), 0, own_partner_ref[...])
    put((3, 0, 4, 1), 0, own_far_ref[...])
    put((0, 1, 3, 4), 0, far_ref[...])

    @pl.when(middle)
    def _():
        put((0, 3, 1, 0), 0, beside_ref[...])

    @pl.when(jnp.logical_and(jnp.logical_not(middle), step == 0))
    def _():
        put((1, 1, 1, 3), 1, rows_ref[...], cross_ref[...])

    @pl.when(jnp.logical_and(jnp.logical_not(middle), step == 1))
    def _():
        low = jnp.concatenate([ends_ref[:across, :], ends_ref[across:, :]], axis=1)
        put((1, 1, 1, 3), 0, low, tiles_ref[...])


def call(kernel, outs, *operands, last=False):
    specs, placed = [], []
    for value in operands:
        scalar = value.dtype == jnp.int32
        specs.append(pl.BlockSpec(memory_space=pltpu.SMEM if scalar else pltpu.VMEM))
        placed.append(value if scalar else pltpu.with_memory_space_constraint(value, pltpu.VMEM))
    return pl.pallas_call(
        kernel,
        out_shape=[jax.ShapeDtypeStruct(*o) if last else pltpu.VMEM(*o) for o in outs],
        in_specs=specs,
        out_specs=[pl.BlockSpec(memory_space=pltpu.VMEM) for _ in outs],
        compiler_params=pltpu.CompilerParams(vmem_limit_bytes=VMEM_LIMIT),
    )(*placed)


def body(embeddings):
    count, width = embeddings.shape
    blocks = lax.axis_size(AXES[0]) * lax.axis_size(AXES[1])
    columns = blocks // 4
    scale = 1.0 / width**0.5
    tiles, half = count // TILE, count // 2
    across, size = half // TILE, half // PARTS
    assert blocks % 8 == 0 and size % STEP == 0

    at = lambda column, turn: column % columns * 4 + turn
    far, swap, even, odd, rows, cross, ends = [], [], [], [], [], [], []
    for q in range(columns):
        far += [(at(q, 1), at(q, 0)), (at(q, 2), at(q, 3))]
        far += [(at(q, 3), at(q + 1, 1)), (at(q, 0), at(q - 1, 2))]
        swap += [(at(q, 0), at(q, 2)), (at(q, 2), at(q, 0)), (at(q, 1), at(q, 3)), (at(q, 3), at(q, 1))]
        beside = q ^ 1
        if q % 2 == 1:
            even += [(at(q, 1), at(q, 2)), (at(q, 2), at(q, 1))]
            odd += [(at(q, 3), at(q + 1, 0)), (at(q, 0), at(q - 1, 3))]
            rows += [(at(q, 1), at(q, 0)), (at(q, 2), at(q, 3))]
            ends += [(at(q, 1), at(q - 1, 3)), (at(q, 2), at(q + 1, 0))]
            ends += [(at(q, 0), at(q, 0)), (at(q, 3), at(q, 3))]
            cross += [(at(q, 3), at(q, 1)), (at(q, 0), at(q, 2))]
            cross += [(at(q, 1), at(beside, 1)), (at(q, 2), at(beside, 2))]
        else:
            cross += [(at(q, 0), at(q - 1, 3)), (at(q, 3), at(q + 1, 0))]
            cross += [(at(q, 1), at(q, 3)), (at(q, 2), at(q, 0))]
            ends += [(at(q, 3), at(q, 1)), (at(q, 0), at(q, 2))]
            ends += [(at(q, 1), at(beside, 1)), (at(q, 2), at(beside, 2))]

    def send(value, pairs):
        return lax.ppermute(value, AXES, pairs)

    role = lax.axis_index(AXES).astype(jnp.int32).reshape(1)
    role, embeddings = lax.optimization_barrier((role, embeddings))
    far_rows = send(embeddings, far)
    partner_rows = send(embeddings, swap)
    piece = ((size, width), BF16)
    unit, own, *odd_parts = call(
        functools.partial(own_kernel, scale),
        [((count, width), BF16), ((tiles, count), F32)] + [piece] * PARTS,
        embeddings,
    )
    odd_parts = [send(part, odd) for part in odd_parts]
    partner, *even_parts = call(partner_kernel, [((count, width), BF16)] + [piece] * PARTS, partner_rows)
    even_parts = [send(part, even) for part in even_parts]
    (own_partner,) = call(functools.partial(pair_kernel, scale), [((tiles, count), F32)], unit, partner)
    far_unit, own_far, far_max, beside_max = call(
        functools.partial(far_kernel, scale),
        [((count, width), BF16)] + [((tiles, count), F32)] * 3,
        role,
        far_rows,
        unit,
        partner,
    )
    far_max = send(far_max, [(b, a) for a, b in far])
    beside_max = send(beside_max, swap)
    column = ((tiles, half), F32)
    done = []
    for i, part in enumerate(even_parts):
        done = call(functools.partial(even_kernel, i * size, scale), [column, column], role, part, far_unit, *done)
    rows_max, ends_max = done
    ends_max = send(ends_max, ends)
    rows_max = send(rows_max, rows)
    done = []
    for i, part in enumerate(odd_parts):
        done = call(
            functools.partial(odd_kernel, i * size, scale), [column, ((across, count), F32)], role, part, unit, *done
        )
    cross_max, half_tiles = done
    cross_max = send(cross_max, cross)
    (out,) = call(
        join_kernel,
        [((OFFSETS * tiles, count), F32)],
        role,
        own,
        own_partner,
        own_far,
        far_max,
        beside_max,
        half_tiles,
        rows_max,
        cross_max,
        ends_max,
        last=True,
    )
    return jnp.transpose(out)


def solution(mesh):
    return jax.shard_map(
        body,
        mesh=mesh,
        in_specs=(P(AXES, None),),
        out_specs=P(AXES, None),
        check_vma=False,
    )
```

```python
import functools

import jax
import jax.numpy as jnp
from jax import lax
from jax.experimental import pallas as pl
from jax.experimental.pallas import tpu as pltpu
from jax.sharding import PartitionSpec as P


AXES = ("blk", "grp")
TILE = 128
STEP = 256
PARTS = 2
OFFSETS = 5
VMEM_LIMIT = 16 << 20
F32, BF16 = jnp.float32, jnp.bfloat16


def unit_of(rows):
    values = rows.astype(F32)
    mean = jnp.mean(values * values, axis=-1, keepdims=True)
    return (values * lax.rsqrt(mean + 1e-06)).astype(BF16)


def scores(left, right):
    return lax.dot_general(left, right, (((1,), (1,)), ((), ())), preferred_element_type=F32)


def best(scale, left, right, right_ref, right_at=0, left_ref=None, left_at=0, left_from=0, same=None):
    rows, keys = left.shape[0], right.shape[0]
    for m in range(0, rows, STEP):
        for n in range(0, keys, STEP):
            s = scores(left[m : m + STEP, :], right[n : n + STEP, :])
            if same is not None and m == n:
                s = jnp.where(same, -jnp.inf, s)
            tiles = jnp.max(s.reshape(STEP // TILE, TILE, STEP), axis=1)
            at = right_at + m // TILE
            right_ref[at : at + STEP // TILE, n : n + STEP] = tiles * scale
            if left_ref is not None:
                for t in range(STEP // TILE):
                    tile = jnp.max(s[:, t * TILE : (t + 1) * TILE], axis=1)
                    at = left_at + n // TILE + t
                    left_ref[at : at + 1, left_from + m : left_from + m + STEP] = tile.reshape(1, STEP) * scale


def place(role_ref):
    turn = lax.rem(role_ref[0], 4)
    step = 1 - lax.rem(lax.div(role_ref[0], 4), 2)
    return turn, step, jnp.logical_or(turn == 1, turn == 2)


def own_kernel(scale, rows_ref, unit_ref, own_ref, *part_refs):
    unit_ref[...] = unit_of(rows_ref[...])
    size = part_refs[0].shape[0]
    for i, part_ref in enumerate(part_refs):
        at = (len(part_refs) + i) * size
        part_ref[...] = unit_ref[at : at + size, :]
    same = lax.broadcasted_iota(jnp.int32, (STEP, STEP), 0) == lax.broadcasted_iota(
        jnp.int32, (STEP, STEP), 1
    )
    best(scale, unit_ref, unit_ref, own_ref, same=same)


def partner_kernel(rows_ref, partner_ref, *part_refs):
    partner_ref[...] = unit_of(rows_ref[...])
    size = part_refs[0].shape[0]
    for i, part_ref in enumerate(part_refs):
        part_ref[...] = partner_ref[i * size : (i + 1) * size, :]


def pair_kernel(scale, unit_ref, partner_ref, max_ref):
    best(scale, partner_ref, unit_ref, max_ref)


def far_kernel(scale, role_ref, rows_ref, unit_ref, partner_ref, far_ref, own_far_ref, far_max_ref, beside_ref):
    middle = place(role_ref)[2]
    far_ref[...] = unit_of(rows_ref[...])
    best(scale, far_ref, unit_ref, own_far_ref, left_ref=far_max_ref)

    @pl.when(jnp.logical_not(middle))
    def _():
        best(scale, far_ref, partner_ref, beside_ref)


def even_kernel(first, scale, role_ref, part_ref, far_ref, *refs):
    _, step, middle = place(role_ref)
    rows_ref, ends_ref = refs[-2:]
    half = far_ref.shape[0] // 2
    at, across = first // TILE, half // TILE

    @pl.when(jnp.logical_and(step == 0, middle))
    def _():
        if first:
            old_rows_ref, old_ends_ref = refs[:2]
            rows_ref[:, :first] = old_rows_ref[:, :first]
            ends_ref[:at, :] = old_ends_ref[:at, :]
            ends_ref[across : across + at, :] = old_ends_ref[across : across + at, :]
        best(scale, part_ref, far_ref.at[:half, :], ends_ref, right_at=at, left_ref=rows_ref, left_from=first)
        best(
            scale, part_ref, far_ref.at[half:, :], ends_ref, right_at=across + at,
            left_ref=rows_ref, left_at=across, left_from=first,
        )


def odd_kernel(first, scale, role_ref, part_ref, unit_ref, *refs):
    _, step, middle = place(role_ref)
    cross_ref, tiles_ref = refs[-2:]
    at = first // TILE

    @pl.when(jnp.logical_and(step == 1, jnp.logical_not(middle)))
    def _():
        if first:
            old_cross_ref, old_tiles_ref = refs[:2]
            cross_ref[:, :first] = old_cross_ref[:, :first]
            tiles_ref[:at, :] = old_tiles_ref[:at, :]
        best(scale, part_ref, unit_ref, tiles_ref, right_at=at, left_ref=cross_ref, left_from=first)


def slot_of(turn, slots):
    slot = slots[0]
    for i in range(1, 4):
        slot = jnp.where(turn == i, slots[i], slot)
    return slot


def join_kernel(role_ref, own_ref, own_partner_ref, own_far_ref, far_ref, beside_ref, out_ref):
    turn, _, _ = place(role_ref)
    tiles = own_ref.shape[0]

    def put(slots, value):
        out_ref[pl.ds(pl.multiple_of(slot_of(turn, slots) * tiles, tiles), tiles), :] = value

    put((2, 2, 2, 2), own_ref[...])
    put((4, 4, 0, 0), own_partner_ref[...])
    put((3, 0, 4, 1), own_far_ref[...])
    put((0, 1, 3, 4), far_ref[...])
    put((1, 3, 1, 3), beside_ref[...])


def late_kernel(role_ref, tiles_ref, rows_ref, cross_ref, ends_ref, joined_ref, out_ref, late_ref, sem):
    turn, step, middle = place(role_ref)
    tiles = late_ref.shape[0]
    across = tiles // 2

    @pl.when(jnp.logical_not(middle))
    def _():
        @pl.when(step == 0)
        def _():
            late_ref[...] = jnp.concatenate([rows_ref[...], cross_ref[...]], axis=1)

        @pl.when(step == 1)
        def _():
            low = jnp.concatenate([ends_ref[:across, :], ends_ref[across:, :]], axis=1)
            late_ref[...] = jnp.concatenate([low, tiles_ref[...]], axis=0)

        at = pl.multiple_of(slot_of(turn, (1, 1, 1, 3)) * tiles, tiles)
        copy = pltpu.make_async_copy(late_ref, out_ref.at[pl.ds(at, tiles), :], sem)
        copy.start()
        copy.wait()


def call(kernel, outs, *operands, last=False):
    specs, placed = [], []
    for value in operands:
        scalar = value.dtype == jnp.int32
        specs.append(pl.BlockSpec(memory_space=pltpu.SMEM if scalar else pltpu.VMEM))
        placed.append(value if scalar else pltpu.with_memory_space_constraint(value, pltpu.VMEM))
    return pl.pallas_call(
        kernel,
        out_shape=[jax.ShapeDtypeStruct(*o) if last else pltpu.VMEM(*o) for o in outs],
        in_specs=specs,
        out_specs=[pl.BlockSpec(memory_space=pltpu.VMEM) for _ in outs],
        compiler_params=pltpu.CompilerParams(vmem_limit_bytes=VMEM_LIMIT),
    )(*placed)


def body(embeddings):
    count, width = embeddings.shape
    blocks = lax.axis_size(AXES[0]) * lax.axis_size(AXES[1])
    columns = blocks // 4
    scale = 1.0 / width**0.5
    tiles, half = count // TILE, count // 2
    across, size = half // TILE, half // PARTS
    assert blocks % 8 == 0 and size % STEP == 0

    at = lambda column, turn: column % columns * 4 + turn
    far, swap, even, odd, rows, cross, ends = [], [], [], [], [], [], []
    for q in range(columns):
        far += [(at(q, 1), at(q, 0)), (at(q, 2), at(q, 3))]
        far += [(at(q, 3), at(q + 1, 1)), (at(q, 0), at(q - 1, 2))]
        swap += [(at(q, 0), at(q, 2)), (at(q, 2), at(q, 0)), (at(q, 1), at(q, 3)), (at(q, 3), at(q, 1))]
        beside = q ^ 1
        if q % 2 == 1:
            even += [(at(q, 1), at(q, 2)), (at(q, 2), at(q, 1))]
            odd += [(at(q, 3), at(q + 1, 0)), (at(q, 0), at(q - 1, 3))]
            rows += [(at(q, 1), at(q, 0)), (at(q, 2), at(q, 3))]
            ends += [(at(q, 1), at(q - 1, 3)), (at(q, 2), at(q + 1, 0))]
            ends += [(at(q, 0), at(q ^ 2, 0)), (at(q, 3), at(q ^ 2, 3))]
            cross += [(at(q, 3), at(q, 1)), (at(q, 0), at(q, 2))]
            cross += [(at(q, 1), at(beside, 1)), (at(q, 2), at(beside, 2))]
        else:
            cross += [(at(q, 0), at(q - 1, 3)), (at(q, 3), at(q + 1, 0))]
            cross += [(at(q, 1), at(q, 3)), (at(q, 2), at(q, 0))]
            ends += [(at(q, 3), at(q, 1)), (at(q, 0), at(q, 2))]
            ends += [(at(q, 1), at(beside, 1)), (at(q, 2), at(beside, 2))]

    def send(value, pairs):
        return lax.ppermute(value, AXES, pairs)

    role = lax.axis_index(AXES).astype(jnp.int32).reshape(1)
    role, embeddings = lax.optimization_barrier((role, embeddings))
    far_rows = send(embeddings, far)
    partner_rows = send(embeddings, swap)
    piece = ((size, width), BF16)
    unit, own, *odd_parts = call(
        functools.partial(own_kernel, scale),
        [((count, width), BF16), ((tiles, count), F32)] + [piece] * PARTS,
        embeddings,
    )
    odd_parts = [send(part, odd) for part in odd_parts]
    partner, *even_parts = call(partner_kernel, [((count, width), BF16)] + [piece] * PARTS, partner_rows)
    even_parts = [send(part, even) for part in even_parts]
    (own_partner,) = call(functools.partial(pair_kernel, scale), [((tiles, count), F32)], unit, partner)
    far_unit, own_far, far_max, beside_max = call(
        functools.partial(far_kernel, scale),
        [((count, width), BF16)] + [((tiles, count), F32)] * 3,
        role,
        far_rows,
        unit,
        partner,
    )
    far_max = send(far_max, [(b, a) for a, b in far])
    beside_max = send(beside_max, swap)
    column = ((tiles, half), F32)
    done = []
    for i, part in enumerate(even_parts):
        done = call(functools.partial(even_kernel, i * size, scale), [column, column], role, part, far_unit, *done)
    rows_max, ends_max = done
    ends_max = send(ends_max, ends)
    rows_max = send(rows_max, rows)
    done = []
    for i, part in enumerate(odd_parts):
        done = call(
            functools.partial(odd_kernel, i * size, scale), [column, ((across, count), F32)], role, part, unit, *done
        )
    cross_max, half_tiles = done
    cross_max = send(cross_max, cross)
    (joined,) = call(
        join_kernel, [((OFFSETS * tiles, count), F32)], role, own, own_partner, own_far, far_max, beside_max, last=True
    )
    near = [pltpu.with_memory_space_constraint(v, pltpu.VMEM) for v in (half_tiles, rows_max, cross_max, ends_max)]
    out = pl.pallas_call(
        late_kernel,
        out_shape=jax.ShapeDtypeStruct(joined.shape, F32),
        in_specs=[pl.BlockSpec(memory_space=pltpu.SMEM)]
        + [pl.BlockSpec(memory_space=pltpu.VMEM)] * 4
        + [pl.BlockSpec(memory_space=pltpu.HBM)],
        out_specs=pl.BlockSpec(memory_space=pltpu.HBM),
        scratch_shapes=[pltpu.VMEM((tiles, count), F32), pltpu.SemaphoreType.DMA],
        input_output_aliases={5: 0},
        compiler_params=pltpu.CompilerParams(vmem_limit_bytes=VMEM_LIMIT),
    )(role, *near, joined)
    return jnp.transpose(out)


def solution(mesh):
    return jax.shard_map(
        body,
        mesh=mesh,
        in_specs=(P(AXES, None),),
        out_specs=P(AXES, None),
        check_vma=False,
    )
```

```python
import functools

import jax
import jax.numpy as jnp
from jax import lax
from jax.experimental import pallas as pl
from jax.experimental.pallas import tpu as pltpu
from jax.sharding import PartitionSpec as P


AXES = ("blk", "grp")
TILE = 128
STEP = 256
PARTS = 2
OFFSETS = 5
VMEM_LIMIT = 16 << 20
F32, BF16 = jnp.float32, jnp.bfloat16


def unit_of(rows):
    values = rows.astype(F32)
    mean = jnp.mean(values * values, axis=-1, keepdims=True)
    return (values * lax.rsqrt(mean + 1e-06)).astype(BF16)


def scores(left, right):
    return lax.dot_general(left, right, (((1,), (1,)), ((), ())), preferred_element_type=F32)


def best(scale, left, right, right_ref, right_at=0, left_ref=None, left_at=0, left_from=0, same=None):
    rows, keys = left.shape[0], right.shape[0]
    for m in range(0, rows, STEP):
        for n in range(0, keys, STEP):
            s = scores(left[m : m + STEP, :], right[n : n + STEP, :])
            if same is not None and m == n:
                s = jnp.where(same, -jnp.inf, s)
            tiles = jnp.max(s.reshape(STEP // TILE, TILE, STEP), axis=1)
            at = right_at + m // TILE
            right_ref[at : at + STEP // TILE, n : n + STEP] = tiles * scale
            if left_ref is not None:
                for t in range(STEP // TILE):
                    tile = jnp.max(s[:, t * TILE : (t + 1) * TILE], axis=1)
                    at = left_at + n // TILE + t
                    left_ref[at : at + 1, left_from + m : left_from + m + STEP] = tile.reshape(1, STEP) * scale


def place(role_ref):
    turn = lax.rem(role_ref[0], 4)
    step = 1 - lax.rem(lax.div(role_ref[0], 4), 2)
    return turn, step, jnp.logical_or(turn == 1, turn == 2)


def own_kernel(scale, rows_ref, unit_ref, own_ref, *part_refs):
    unit_ref[...] = unit_of(rows_ref[...])
    size = part_refs[0].shape[0]
    for i, part_ref in enumerate(part_refs):
        at = (len(part_refs) + i) * size
        part_ref[...] = unit_ref[at : at + size, :]
    same = lax.broadcasted_iota(jnp.int32, (STEP, STEP), 0) == lax.broadcasted_iota(
        jnp.int32, (STEP, STEP), 1
    )
    best(scale, unit_ref, unit_ref, own_ref, same=same)


def partner_kernel(rows_ref, partner_ref, *part_refs):
    partner_ref[...] = unit_of(rows_ref[...])
    size = part_refs[0].shape[0]
    for i, part_ref in enumerate(part_refs):
        part_ref[...] = partner_ref[i * size : (i + 1) * size, :]


def pair_kernel(scale, unit_ref, partner_ref, max_ref):
    best(scale, partner_ref, unit_ref, max_ref)


def far_kernel(scale, role_ref, rows_ref, unit_ref, partner_ref, far_ref, own_far_ref, far_max_ref, first_ref):
    middle = place(role_ref)[2]
    far_ref[...] = unit_of(rows_ref[...])
    best(scale, far_ref, unit_ref, own_far_ref, left_ref=far_max_ref)

    @pl.when(jnp.logical_not(middle))
    def _():
        best(scale, far_ref, partner_ref, first_ref)

    @pl.when(middle)
    def _():
        first_ref[...] = far_max_ref[...]


def even_kernel(first, scale, role_ref, part_ref, far_ref, far_max_ref, *refs):
    _, step, middle = place(role_ref)
    rows_ref, ends_ref = refs[-2:]
    half = far_ref.shape[0] // 2
    at, across = first // TILE, half // TILE

    @pl.when(jnp.logical_not(middle))
    def _():
        rows_ref[...] = far_max_ref[...]

    @pl.when(jnp.logical_and(step == 0, middle))
    def _():
        if first:
            old_rows_ref, old_ends_ref = refs[:2]
            rows_ref[:, :first] = old_rows_ref[:, :first]
            ends_ref[:at, :] = old_ends_ref[:at, :]
            ends_ref[across : across + at, :] = old_ends_ref[across : across + at, :]
        best(scale, part_ref, far_ref.at[:half, :], ends_ref, right_at=at, left_ref=rows_ref, left_from=first)
        best(
            scale, part_ref, far_ref.at[half:, :], ends_ref, right_at=across + at,
            left_ref=rows_ref, left_at=across, left_from=first,
        )


def odd_kernel(first, scale, role_ref, part_ref, unit_ref, *refs):
    _, step, middle = place(role_ref)
    cross_ref, tiles_ref = refs[-2:]
    at = first // TILE

    @pl.when(jnp.logical_and(step == 1, jnp.logical_not(middle)))
    def _():
        if first:
            old_cross_ref, old_tiles_ref = refs[:2]
            cross_ref[:, :first] = old_cross_ref[:, :first]
            tiles_ref[:at, :] = old_tiles_ref[:at, :]
        best(scale, part_ref, unit_ref, tiles_ref, right_at=at, left_ref=cross_ref, left_from=first)


def join_kernel(
    role_ref, own_ref, own_partner_ref, own_far_ref, first_ref, tiles_ref, rows_ref, cross_ref,
    ends_ref, out_ref
):
    turn, step, middle = place(role_ref)
    tiles, count = own_ref.shape
    across = tiles // 2

    def put(slots, *values):
        slot = slots[0]
        for i in range(1, 4):
            slot = jnp.where(turn == i, slots[i], slot)
        at = pl.multiple_of(slot * tiles, tiles)
        out_ref[pl.ds(at, tiles), :] = jnp.concatenate(values[1:], axis=values[0])

    put((2, 2, 2, 2), 0, own_ref[...])
    put((4, 4, 0, 0), 0, own_partner_ref[...])
    put((3, 0, 4, 1), 0, own_far_ref[...])
    put((0, 3, 1, 4), 0, first_ref[...])

    @pl.when(middle)
    def _():
        put((0, 1, 3, 0), 0, rows_ref[...])

    @pl.when(jnp.logical_and(jnp.logical_not(middle), step == 0))
    def _():
        put((1, 1, 1, 3), 1, rows_ref[:, : count // 2], cross_ref[...])

    @pl.when(jnp.logical_and(jnp.logical_not(middle), step == 1))
    def _():
        low = jnp.concatenate([ends_ref[:across, :], ends_ref[across:, :]], axis=1)
        put((1, 1, 1, 3), 0, low, tiles_ref[...])


def call(kernel, outs, *operands, last=False):
    specs, placed = [], []
    for value in operands:
        scalar = value.dtype == jnp.int32
        specs.append(pl.BlockSpec(memory_space=pltpu.SMEM if scalar else pltpu.VMEM))
        placed.append(value if scalar else pltpu.with_memory_space_constraint(value, pltpu.VMEM))
    return pl.pallas_call(
        kernel,
        out_shape=[jax.ShapeDtypeStruct(*o) if last else pltpu.VMEM(*o) for o in outs],
        in_specs=specs,
        out_specs=[pl.BlockSpec(memory_space=pltpu.VMEM) for _ in outs],
        compiler_params=pltpu.CompilerParams(vmem_limit_bytes=VMEM_LIMIT),
    )(*placed)


def body(embeddings):
    count, width = embeddings.shape
    blocks = lax.axis_size(AXES[0]) * lax.axis_size(AXES[1])
    columns = blocks // 4
    scale = 1.0 / width**0.5
    tiles, half = count // TILE, count // 2
    across, size = half // TILE, half // PARTS
    assert blocks % 8 == 0 and size % STEP == 0

    at = lambda column, turn: column % columns * 4 + turn
    far, first, swap, even, odd, rows, cross, ends = [], [], [], [], [], [], [], []
    for q in range(columns):
        far += [(at(q, 1), at(q, 0)), (at(q, 2), at(q, 3))]
        far += [(at(q, 3), at(q + 1, 1)), (at(q, 0), at(q - 1, 2))]
        swap += [(at(q, 0), at(q, 2)), (at(q, 2), at(q, 0)), (at(q, 1), at(q, 3)), (at(q, 3), at(q, 1))]
        beside = q ^ 1
        rows += [(at(q, 0), at(q, 1)), (at(q, 3), at(q, 2))]
        first += [(at(q, 1), at(q - 1, 3)), (at(q, 2), at(q + 1, 0)), (at(q, 0), at(q, 2)), (at(q, 3), at(q, 1))]
        if q % 2 == 1:
            even += [(at(q, 1), at(q, 2)), (at(q, 2), at(q, 1))]
            odd += [(at(q, 3), at(q + 1, 0)), (at(q, 0), at(q - 1, 3))]
            ends += [(at(q, 1), at(q - 1, 3)), (at(q, 2), at(q + 1, 0))]
            rows += [(at(q, 1), at(q, 0)), (at(q, 2), at(q, 3))]
            ends += [(at(q, 0), at(q, 3)), (at(q, 3), at(q, 0))]
            cross += [(at(q, 3), at(q, 1)), (at(q, 0), at(q, 2))]
            cross += [(at(q, 1), at(beside, 1)), (at(q, 2), at(beside, 2))]
        else:
            cross += [(at(q, 0), at(q - 1, 3)), (at(q, 3), at(q + 1, 0))]
            rows += [(at(q, 1), at(q, 3)), (at(q, 2), at(q, 0))]
            cross += [(at(q, 1), at(q, 3)), (at(q, 2), at(q, 0))]
            ends += [(at(q, 3), at(q, 1)), (at(q, 0), at(q, 2))]
            ends += [(at(q, 1), at(beside, 1)), (at(q, 2), at(beside, 2))]

    def send(value, pairs):
        return lax.ppermute(value, AXES, pairs)

    role = lax.axis_index(AXES).astype(jnp.int32).reshape(1)
    role, embeddings = lax.optimization_barrier((role, embeddings))
    far_rows = send(embeddings, far)
    partner_rows = send(embeddings, swap)
    piece = ((size, width), BF16)
    unit, own, *odd_parts = call(
        functools.partial(own_kernel, scale),
        [((count, width), BF16), ((tiles, count), F32)] + [piece] * PARTS,
        embeddings,
    )
    odd_parts = [send(part, odd) for part in odd_parts]
    partner, *even_parts = call(partner_kernel, [((count, width), BF16)] + [piece] * PARTS, partner_rows)
    even_parts = [send(part, even) for part in even_parts]
    (own_partner,) = call(functools.partial(pair_kernel, scale), [((tiles, count), F32)], unit, partner)
    far_unit, own_far, far_max, first_max = call(
        functools.partial(far_kernel, scale),
        [((count, width), BF16)] + [((tiles, count), F32)] * 3,
        role,
        far_rows,
        unit,
        partner,
    )
    first_max = send(first_max, first)
    column = ((tiles, half), F32)
    done = []
    for i, part in enumerate(even_parts):
        done = call(
            functools.partial(even_kernel, i * size, scale), [((tiles, count), F32), column],
            role, part, far_unit, far_max, *done
        )
    rows_max, ends_max = done
    ends_max = send(ends_max, ends)
    done = []
    for i, part in enumerate(odd_parts):
        done = call(
            functools.partial(odd_kernel, i * size, scale), [column, ((across, count), F32)], role, part, unit, *done
        )
    cross_max, half_tiles = done
    cross_max = send(cross_max, cross)
    rows_max = send(rows_max, rows)
    (out,) = call(
        join_kernel,
        [((OFFSETS * tiles, count), F32)],
        role,
        own,
        own_partner,
        own_far,
        first_max,
        half_tiles,
        rows_max,
        cross_max,
        ends_max,
        last=True,
    )
    return jnp.transpose(out)


def solution(mesh):
    return jax.shard_map(
        body,
        mesh=mesh,
        in_specs=(P(AXES, None),),
        out_specs=P(AXES, None),
        check_vma=False,
    )
```
